128 devices in a mesh: expert: 32 (over z, y, x_hi), mp: 4 (over x_lo, core).
Axes of the slice: x: 4 (x_hi: 2, x_lo: 2; x = x_hi * 2 + x_lo), y: 4, z: 4, core: 2. Of those that a mesh axis runs over, the one named last changes fastest.
Arguments:
- queries: bfloat16 [1024, 48, 128], P('expert', 'mp'), may hold values from -140 to 140
- k_cache: bfloat16 [1024, 8, 128, 128], P('expert', 'mp'), may hold values from -5 to 5
- v_cache: bfloat16 [1024, 8, 128, 128], P('expert', 'mp'), may hold values from -6 to 6
- lengths: int32 [1024], P('expert'), may hold values from 2 to 128
- moe_input: bfloat16 [1024, 6144], P('expert', 'mp'), may hold values from -40 to 40
- norm_gain: float32 [6144], P('mp'), may hold values from 0.5 to 1.5
- expert_ids: int32 [1024, 2], P('expert'), may hold values from 0 to 7, all different within a row; in each aligned block of 32 rows (0 to 31, 32 to 63, ...) at most 16 rows name the same one
- combine_weights: float32 [1024, 2], P('expert'), may hold values from 0.1 to 1
- capacity: int32 [8], replicated, may hold values from 8 to 16
- w_gate: bfloat16 [32, 6144, 2048], P('expert', None, 'mp'), may hold values from -0.078125 to 0.078125
- w_up: bfloat16 [32, 6144, 2048], P('expert', None, 'mp'), may hold values from -0.078125 to 0.078125
- w_down: bfloat16 [32, 2048, 6144], P('expert', 'mp'), may hold values from -0.0625 to 0.0625
Outputs:
- context: bfloat16 [1024, 48, 128], P('expert', 'mp')
- layer_out: bfloat16 [1024, 6144], P('expert', 'mp')
The draws below stay inside these ranges and needn't reach their ends.
Inputs may be any that keep to these rules, and one draw needn't show every extreme that they name: `expert_ids`: within each aligned block of 32 tokens, no expert is named by more than 16 tokens; the 2 ids of a token differ.
All inputs are finite; a program needn't handle non-finite values.
Results may differ from the reference program's by a relative error of at most 0.007.
Values may be sent and summed in bfloat16 or wider, within the bound.
A program may use at most 128 MiB of HBM per device.

```python
import math
import jax
import jax.numpy as jnp
import numpy as np
from jax import lax

D = 6144
HEADS = 48
KV_HEADS = 8
HEAD_DIM = 128
FFW = 8192
EXPERTS = 8
TOP = 2
TOK_DEV = 32
LMAX = 128
CAP = 16
SPLIT = 4
TOKENS = 1024
BATCH = 1024
N_EXPERT = 32


def key_table(key):
    keys = jnp.clip(jax.random.normal(jax.random.fold_in(key, 11), (BATCH, KV_HEADS, LMAX, HEAD_DIM), jnp.float32), -5.0, 5.0)
    return keys


def draw_k_cache(key, part):
    return key_table(key).astype(jnp.bfloat16)


def draw_queries(key, part):
    values = jnp.clip(jax.random.normal(jax.random.fold_in(key, 23), (BATCH, HEADS, HEAD_DIM), jnp.float32), -5.0, 5.0)
    return values.astype(jnp.bfloat16)


def draw_moe_input(key, part):
    base = jnp.clip(jax.random.normal(jax.random.fold_in(key, 5), (TOKENS, D), jnp.float32), -4.0, 4.0)
    rough = jax.random.uniform(jax.random.fold_in(key, 6), (D,), jnp.float32, 0.8, 1.25)
    column = 0.25 * 10.0 ** (jnp.arange(D).astype(jnp.float32) / D) * rough
    values = base * column[None, :]
    return values.astype(jnp.bfloat16)


def plant(array, rng, low, largest):
    longest = array.shape.index(max(array.shape))
    spots = []
    for shift in (0, 1):
        where = [jax.random.randint(jax.random.fold_in(rng, axis), (), 0, length) for axis, length in enumerate(array.shape)]
        where[longest] = (where[longest] + shift) % array.shape[longest]
        spots.append(tuple(where))
    return array.at[spots[0]].set(low).at[spots[1]].set(largest)


def block_levels(own_key, dims, pieces, least, largest):
    level = 1.0
    for dim, parts in pieces:
        draws = jax.random.uniform(jax.random.fold_in(jax.random.fold_in(own_key, 6), dim), (parts,), jnp.float32, least / len(pieces), largest / len(pieces))
        level = level * jnp.repeat(jnp.exp(draws), dims[dim] // parts).reshape((-1,) + (1,) * (len(dims) - 1 - dim))
    return level


def shared_out(rng, own, number, rows, number_of, top, limit, lean):
    ranking = jax.random.permutation(rng, number_of)
    heavy_load, usual = shares(number_of, rows * top, limit, lean, True), shares(number_of, rows * top, limit, lean, False)
    places = jnp.arange(number_of)

    def named(tallies, offset_by):
        used = int((tallies > 0).sum())
        fixed = max(1, used // 4)
        shifted = fixed + (places - fixed + offset_by * (used - fixed)) % max(1, number_of - fixed)
        return jnp.zeros((number_of,), jnp.int32).at[ranking[jnp.where(places < fixed, places, shifted)]].set(jnp.asarray(tallies, jnp.int32))

    tallies = jnp.where(number % 4 == 0, named(heavy_load, number // 4), named(usual, number - number // 4 - 1))
    mixed = jax.random.permutation(jax.random.fold_in(own, 3), number_of)
    giver, receiver = mixed[0:number_of // 2 * 2:2], mixed[1:number_of // 2 * 2:2]
    slack = jnp.minimum(tallies[giver] - 1, limit - tallies[receiver]) // 2
    slack = jnp.where((giver == ranking[0]) | (receiver == ranking[0]) | (tallies[receiver] == 0), 0, jnp.maximum(slack, 0))
    shifted = jax.random.randint(jax.random.fold_in(own, 4), (number_of // 2,), 0, 1 << 20) % (slack + 1)
    tallies = tallies.at[giver].add(-shifted).at[receiver].add(shifted)
    members = jnp.searchsorted(jnp.cumsum(tallies), jnp.arange(rows * top), side="right").astype(jnp.int32)
    grid = members.reshape(top, rows).T
    grid = grid[jax.random.permutation(jax.random.fold_in(own, 1), rows)]
    offset_by = jax.random.randint(jax.random.fold_in(own, 2), (rows, 1), 0, top)
    return jnp.take_along_axis(grid, (jnp.arange(top)[None, :] + offset_by) % top, axis=1)


def shares(amount, total, bound, slope, full):
    loads = [(1 << 20) // math.isqrt(rank ** slope) + 1 for rank in range(1, amount + 1)]
    largest = bound if full else min(bound, max(-(-total // amount), total * loads[0] // sum(loads)))
    least = 1 if total - largest >= amount - 1 else 0
    holding, spare = [largest] + [least] * (amount - 1), total - largest - least * (amount - 1)
    while spare > 0:
        movable = [i for i in range(1, amount) if holding[i] < largest] or [i for i in range(1, amount) if holding[i] < bound]
        mass, left = sum([loads[i] for i in movable]), spare
        for i in movable:
            extra = min(bound - holding[i], max(1, left * loads[i] // mass), spare)
            holding[i] = holding[i] + extra
            spare = spare - extra
    return np.array(holding)


def scatter_about(own_key, extent, deviation, bound, shards=(), dtype=jnp.bfloat16):
    entries = jax.random.normal(own_key, extent, jnp.float32) * deviation
    if len(shards) > 0:
        entries = block_levels(own_key, extent, shards, -0.22, 0.18) * entries
    return jnp.clip(entries, min=-bound, max=bound).astype(dtype)


def setup_inputs(seed: int = 0) -> dict:
    streams_of = jax.random.split(jax.random.key(seed), 13)
    queries = draw_queries(jax.random.fold_in(streams_of[12], 71), 0)
    k_cache = draw_k_cache(jax.random.fold_in(streams_of[12], 71), 0)
    v_cache = scatter_about(streams_of[2], (BATCH, KV_HEADS, LMAX, HEAD_DIM), 1.0, 6.0, ((0, 32), (1, 4)))
    lengths = plant(jax.random.randint(streams_of[3], (BATCH,), 2, LMAX + 1), jax.random.fold_in(streams_of[3], 1), 2, LMAX).astype(jnp.int32)
    moe_input = draw_moe_input(jax.random.fold_in(streams_of[12], 71), 0)
    norm_gain = jnp.clip(1.0 + 0.1 * jax.random.normal(streams_of[5], (D,), jnp.float32), 0.5, 1.5)
    expert_ids_keys = jax.random.split(jax.random.fold_in(streams_of[6], 1), TOKENS // TOK_DEV)
    expert_ids_turns = jax.random.permutation(jax.random.fold_in(streams_of[6], 3), TOKENS // TOK_DEV)
    expert_ids = jax.vmap(lambda own, number: shared_out(jax.random.fold_in(streams_of[6], 2), own, number, TOK_DEV, EXPERTS, TOP, CAP, 2))(expert_ids_keys, expert_ids_turns).reshape((TOKENS, TOP))
    combine_weights = jnp.clip(0.1 + 0.9 * jax.random.uniform(streams_of[7], (TOKENS, TOP), jnp.float32) ** block_levels(streams_of[7], (TOKENS, TOP), ((0, 32),), -0.2, 0.2), 0.1, 1.0)
    capacity = plant(jax.random.randint(streams_of[8], (EXPERTS,), CAP // 2, CAP + 1), jax.random.fold_in(streams_of[8], 1), CAP // 2, CAP).astype(jnp.int32)
    w_gate = scatter_about(streams_of[9], (EXPERTS * SPLIT, D, FFW // SPLIT), D ** -0.5, 0.078125, ((0, 32), (2, 4)))
    w_up = scatter_about(streams_of[10], (EXPERTS * SPLIT, D, FFW // SPLIT), D ** -0.5, 0.078125, ((0, 32), (2, 4)))
    w_down = scatter_about(streams_of[11], (EXPERTS * SPLIT, FFW // SPLIT, D), FFW ** -0.5, 0.0625, ((0, 32), (1, 4)))
    return {"queries": queries, "k_cache": k_cache, "v_cache": v_cache, "lengths": lengths, "moe_input": moe_input, "norm_gain": norm_gain, "expert_ids": expert_ids, "combine_weights": combine_weights, "capacity": capacity, "w_gate": w_gate, "w_up": w_up, "w_down": w_down}


def reference(queries, k_cache, v_cache, lengths, moe_input, norm_gain, expert_ids, combine_weights, capacity, w_gate, w_up, w_down):
    group_size = HEADS // KV_HEADS
    queries_grouped = queries.astype(jnp.float32).reshape(BATCH, KV_HEADS, group_size, HEAD_DIM)
    scores = jnp.einsum('bjgd,bjpd->bjgp', queries_grouped, k_cache.astype(jnp.float32)) * HEAD_DIM ** (-0.5)
    live_mask = jnp.arange(LMAX).astype(jnp.int32)[None, :] < lengths[:, None]
    scores = jnp.where(live_mask[:, None, None, :], scores, -jnp.inf)
    top_score = lax.optimization_barrier(jnp.max(scores, axis=-1, keepdims=True))
    expo = jnp.exp(scores - top_score)
    probs = (expo / lax.optimization_barrier(jnp.sum(expo, axis=-1, keepdims=True))).astype(jnp.bfloat16)
    context = jnp.einsum('bjgp,bjpd->bjgd', probs.astype(jnp.float32), v_cache.astype(jnp.float32))
    context = context.astype(jnp.bfloat16).reshape(BATCH, HEADS, HEAD_DIM)
    residual = moe_input.astype(jnp.float32)
    mean_square = lax.optimization_barrier(jnp.mean(residual * residual, axis=-1))
    normed = (residual * lax.rsqrt(mean_square + 1e-05)[:, None] * norm_gain[None, :]).astype(jnp.bfloat16)
    flat_ids = expert_ids.reshape(-1)
    one_hot = (flat_ids[:, None] == jnp.arange(EXPERTS).astype(jnp.int32)[None, :]).astype(jnp.int32)
    blocked = one_hot.reshape(N_EXPERT, TOK_DEV * TOP, EXPERTS)
    earlier = (jnp.cumsum(blocked, axis=1).astype(jnp.int32) - blocked).reshape(-1, EXPERTS)
    slot_rank = lax.optimization_barrier(jnp.sum(earlier * one_hot, axis=1)).astype(jnp.int32)
    limits = lax.optimization_barrier(jnp.sum(one_hot * capacity[None, :], axis=1)).astype(jnp.int32)
    kept_mask = slot_rank < limits
    token_index = (jnp.arange(TOKENS * TOP) // TOP).astype(jnp.int32)
    source = (token_index // TOK_DEV).astype(jnp.int32)
    slot_id = (source * CAP + slot_rank).astype(jnp.int32)
    dropped_slot = jnp.where(kept_mask, slot_id, N_EXPERT * CAP).astype(jnp.int32)
    table = jnp.zeros((EXPERTS, N_EXPERT * CAP), jnp.int32).at[flat_ids, dropped_slot].set(token_index, mode='drop')
    filled = jnp.zeros((EXPERTS, N_EXPERT * CAP), jnp.int32).at[flat_ids, dropped_slot].set(1, mode='drop')
    piece_width = FFW // SPLIT
    gate_pieces = w_gate.reshape(EXPERTS, SPLIT, D, piece_width)
    up_pieces = w_up.reshape(EXPERTS, SPLIT, D, piece_width)
    down_rows = w_down.reshape(EXPERTS, FFW, D)

    def expert_block(operands):
        row_index, row_filled, gate_w, up_w, down_w = operands
        picked = jnp.where(row_filled[:, None] > 0, normed[row_index], jnp.zeros((), jnp.bfloat16))
        gate_sum = jnp.concatenate([jnp.dot(picked, gate_w[piece], preferred_element_type=jnp.float32) for piece in range(SPLIT)], axis=1)
        up_sum = jnp.concatenate([jnp.dot(picked, up_w[piece], preferred_element_type=jnp.float32) for piece in range(SPLIT)], axis=1)
        hidden = (jax.nn.silu(gate_sum) * up_sum).astype(jnp.bfloat16)
        return jnp.dot(hidden, down_w, preferred_element_type=jnp.float32)
    expert_out = lax.map(expert_block, (table, filled, gate_pieces, up_pieces, down_rows))
    safe_slot = jnp.where(kept_mask, slot_id, 0).astype(jnp.int32)
    chosen_out = expert_out[flat_ids, safe_slot]
    coefficient = combine_weights.reshape(-1) * kept_mask.astype(jnp.float32)
    added = (chosen_out * coefficient[:, None]).reshape(TOKENS, TOP, D).sum(axis=1)
    layer_out = (residual + added).astype(jnp.bfloat16)
    return (context, layer_out)
```

```python
import jax
import jax.numpy as jnp
from jax import lax
from jax.experimental import pallas as pl
from jax.experimental.pallas import tpu as pltpu
from jax.sharding import PartitionSpec as P

MESH = pl.DeviceIdType.MESH
F32 = jnp.float32
BF16 = jnp.bfloat16

D = 6144
EXPERTS = 8
SLOTS = 16
TOK = 32
FEAT = 1536
HID = 512
ROWS = 512
SEQS = 32
STEP = (0, 1, 3, 2)


def base(h, p):
    return (p // 2) * 256 + h * 128 + (p % 2) * 64


def kernel(
    lengths,
    capacity,
    q_ref,
    x_ref,
    gain_ref,
    ids_ref,
    wts_ref,
    k_hbm,
    v_hbm,
    wg_hbm,
    wu_hbm,
    wd_hbm,
    ctx_ref,
    out_ref,
    kv,
    vv,
    wg,
    wu,
    wd,
    xb,
    pk,
    acc_g,
    acc_u,
    hid,
    ps,
    pr,
    q1,
    q0,
    xr,
    own,
    rb,
    sq,
    rt,
    nm,
    fin,
    w_sem,
    kv_sem,
    sq_s,
    sq_r,
    rt_s,
    rt_r,
    nm_s,
    nm_r,
    s1_s,
    s1_r,
    xf_s,
    xf_r,
    dd_s,
    dd_r,
    pr_s,
    pr_r,
    xq_s,
    xq_r,
    r2_s,
    r2_r,
    fin_s,
    fin_r,
):
    s = lax.axis_index("expert")
    m = lax.axis_index("mp")
    z = s // 8
    y = (s // 2) % 4
    s_other = s + 1 - 2 * (s % 2)
    m_core = m + 1 - 2 * (m % 2)
    m_near = (m + 2) % 4
    m_both = 3 - m
    mates = (m, m_core, m_near, m_both)
    x_hi = s % 2
    mate = (s, m_core)
    near = (s, m_near)
    far = (s_other, m_near)
    opp = (s_other, m)

    def plane(dz, dy):
        return (((z + dz) % 4) * 8 + ((y + dy) % 4) * 2 + x_hi, m)

    def send(src, dst, send_sem, recv_sem, device):
        pltpu.make_async_remote_copy(
            src_ref=src,
            dst_ref=dst,
            send_sem=send_sem,
            recv_sem=recv_sem,
            device_id=device,
            device_id_type=MESH,
        ).start()

    def wait(ref, sem):
        pltpu.make_async_copy(ref, ref, sem).wait()

    copies = []
    for k in range(4):
        rows = pl.ds(pl.multiple_of(mates[k] * FEAT, FEAT), FEAT)
        copies.append(pltpu.make_async_copy(wg_hbm.at[0, rows, :], wg.at[k], w_sem.at[0, k]))
        copies.append(pltpu.make_async_copy(wu_hbm.at[0, rows, :], wu.at[k], w_sem.at[1, k]))
        copies.append(pltpu.make_async_copy(wd_hbm.at[0, :, rows], wd.at[k], w_sem.at[2, k]))
    k_copy = pltpu.make_async_copy(k_hbm, kv, kv_sem.at[0])
    v_copy = pltpu.make_async_copy(v_hbm, vv, kv_sem.at[1])
    k_copy.start()
    v_copy.start()
    for copy in copies:
        copy.start()

    barrier = pltpu.get_barrier_semaphore()
    partners = [plane(dz, dy) for dz in range(4) for dy in range(4) if (dz, dy) != (0, 0)]
    partners += [mate, near, far, opp, (s, m_both)]
    for device in partners:
        pl.semaphore_signal(barrier, inc=1, device_id=device, device_id_type=MESH)

    lane = lax.broadcasted_iota(jnp.int32, (TOK, 128), 1)
    ids = ids_ref[...].astype(F32)
    wts = wts_ref[...]
    route = jnp.where(
        lane == 0,
        ids[:, 0:1],
        jnp.where(lane == 1, ids[:, 1:2], jnp.where(lane == 2, wts[:, 0:1], wts[:, 1:2])),
    )
    rt[0] = route
    x = x_ref[...].astype(F32)
    mine = jnp.sum(x * x, axis=1, keepdims=True)
    sq[0] = jnp.broadcast_to(mine, (TOK, 128))

    pl.semaphore_wait(barrier, len(partners))
    for k in range(1, 4):
        send(sq.at[0], sq.at[k], sq_s, sq_r.at[k], (s, mates[k]))
    send(rt.at[0], rt.at[1], rt_s, rt_r, opp)

    col = lax.broadcasted_iota(jnp.int32, (TOK, 256), 1)
    group = col // 64
    dz_col = jnp.where(group == 3, 2, jnp.where(group == 2, 3, group))
    e_col = ((z + dz_col) % 4) * 2 + ((y + (col // 16) % 4) % 4) // 2
    j_col = col % 16
    cap_col = jnp.zeros((TOK, 256), jnp.int32)
    for e in range(EXPERTS):
        cap_col = jnp.where(e_col == e, capacity[e], cap_col)
    open_col = j_col < cap_col
    e_col_f = e_col.astype(F32)
    j_col_f = j_col.astype(F32)
    tri = (
        lax.broadcasted_iota(jnp.int32, (TOK, TOK), 1)
        < lax.broadcasted_iota(jnp.int32, (TOK, TOK), 0)
    ).astype(F32).astype(BF16)

    def routing(route):
        first = route[:, 0:1] == e_col_f
        second = route[:, 1:2] == e_col_f
        member = first | second
        rank = jnp.dot(tri, member.astype(F32).astype(BF16), preferred_element_type=F32)
        take = member & (rank == j_col_f) & open_col
        weight = jnp.where(take, jnp.where(first, route[:, 2:3], route[:, 3:4]), 0.0)
        return take.astype(F32).astype(BF16), weight

    take_own, weight_own = routing(route)

    for k in range(1, 4):
        wait(sq.at[k], sq_r.at[k])
    total = (sq[0] + sq[1] + sq[2] + sq[3])[:, 0:1]
    normed = (x * lax.rsqrt(total / D + 1e-05) * gain_ref[...]).astype(BF16)
    nm[0] = normed
    send(nm.at[0], nm.at[1], nm_s, nm_r, opp)

    def pack(h, take, features):
        packed = lax.dot_general(
            take, features, (((0,), (0,)), ((), ())), preferred_element_type=F32
        ).astype(BF16)
        pk[h] = packed
        xb[0, 0, base(h, 0) : base(h, 0) + SLOTS, :] = packed[0:SLOTS, :]
        for p in range(4):
            for dy in range(4):
                if p == 0 and dy == 0:
                    continue
                at = base(h, p) + dy * SLOTS
                send(
                    pk.at[h, pl.ds(p * 64 + dy * SLOTS, SLOTS), :],
                    xb.at[0, 0, pl.ds(at, SLOTS), :],
                    s1_s.at[h],
                    s1_r.at[h, p],
                    plane(STEP[p], dy),
                )

    def wait_slots(h, p):
        if p == 0:
            wait(xb.at[0, 0, pl.ds(base(h, p) + SLOTS, 48), :], s1_r.at[h, p])
        else:
            wait(xb.at[0, 0, pl.ds(base(h, p), 64), :], s1_r.at[h, p])

    def to_mate(kx, h, p):
        rows = pl.ds(base(h, p), 64)
        send(xb.at[kx, 0, rows, :], xb.at[kx, 1, rows, :], dd_s.at[kx], dd_r.at[kx, p // 2], mate)

    def forward_own(p):
        wait_slots(0, p)
        rows = pl.ds(base(0, p), 64)
        send(xb.at[0, 0, rows, :], xb.at[1, 0, rows, :], xf_s.at[0], xf_r.at[0, p], near)
        send(
            xb.at[0, 0, rows, :],
            xb.at[1, 0, pl.ds(base(1, p), 64), :],
            xf_s.at[1],
            xf_r.at[1, p],
            far,
        )
        to_mate(0, 0, p)

    def forward_opp(p):
        wait_slots(1, p)
        to_mate(0, 1, p)

    def forward_side(p):
        for h in range(2):
            wait(xb.at[1, 0, pl.ds(base(h, p), 64), :], xf_r.at[h, p])
            to_mate(1, h, p)

    position = lax.broadcasted_iota(jnp.int32, (12, 256), 1)
    head = lax.broadcasted_iota(jnp.int32, (12, 128), 0)
    low_head = head < 6
    position = position[:, 0:128]

    def attend(b):
        scores = lax.dot_general(
            q_ref[b],
            kv[b].reshape(256, 128),
            (((1,), (1,)), ((), ())),
            preferred_element_type=F32,
        )
        scores = jnp.where(low_head, scores[:, 0:128], scores[:, 128:256]) * 128 ** (-0.5)
        scores = jnp.where(position < lengths[b], scores, -jnp.inf)
        expo = jnp.exp(scores - jnp.max(scores, axis=1, keepdims=True))
        probs = expo / jnp.sum(expo, axis=1, keepdims=True)
        both = jnp.concatenate(
            [jnp.where(low_head, probs, 0.0), jnp.where(low_head, 0.0, probs)], axis=1
        ).astype(BF16)
        ctx_ref[b] = jnp.dot(
            both, vv[b].reshape(256, 128), preferred_element_type=F32
        ).astype(BF16)

    def attention(first, count):
        def some(i, carry):
            for u in range(8):
                attend(first + i * 8 + u)
            return carry

        lax.fori_loop(0, count // 8, some, 0)

    pack(0, take_own, normed)
    k_copy.wait()
    v_copy.wait()
    attention(0, 8)
    wait(rt.at[1], rt_r)
    take_opp, weight_opp = routing(rt[1])
    forward_own(0)
    wait(nm.at[1], nm_r)
    pack(1, take_opp, nm[1])
    forward_own(1)
    attention(8, 8)
    forward_own(2)
    forward_opp(0)
    attention(16, 8)
    forward_own(3)
    forward_opp(1)
    forward_side(0)
    attention(24, 8)

    def gate_up(k, half):
        kx, cc = k // 2, k % 2
        rows = pl.ds(half * 256, 256)
        for n in range(2):
            cols = pl.ds(n * 256, 256)
            g = jnp.dot(xb[kx, cc, rows, :], wg[k, :, cols], preferred_element_type=F32)
            u = jnp.dot(xb[kx, cc, rows, :], wu[k, :, cols], preferred_element_type=F32)
            if k != 0:
                g = g + acc_g[rows, cols]
                u = u + acc_u[rows, cols]
            if k != 3:
                acc_g[rows, cols] = g
                acc_u[rows, cols] = u
            else:
                hid[rows, cols] = (g / (1.0 + jnp.exp(-g)) * u).astype(BF16)

    def weights(kind, k):
        copies[k * 3 + kind].wait()

    weights(0, 0)
    weights(1, 0)
    gate_up(0, 0)
    forward_opp(2)
    forward_side(1)
    weights(0, 1)
    weights(1, 1)
    wait(xb.at[0, 1, pl.ds(0, 256), :], dd_r.at[0, 0])
    gate_up(1, 0)
    forward_opp(3)
    gate_up(0, 1)
    weights(0, 2)
    weights(1, 2)
    gate_up(2, 0)
    forward_side(2)
    wait(xb.at[0, 1, pl.ds(256, 256), :], dd_r.at[0, 1])
    gate_up(1, 1)
    weights(0, 3)
    weights(1, 3)
    wait(xb.at[1, 1, pl.ds(0, 256), :], dd_r.at[1, 0])
    gate_up(3, 0)
    forward_side(3)
    gate_up(2, 1)
    wait(xb.at[1, 1, pl.ds(256, 256), :], dd_r.at[1, 1])
    gate_up(3, 1)

    def down(k, half, n):
        return jnp.dot(
            hid[half * 256 : half * 256 + 256, :],
            wd[k, :, n * 512 : n * 512 + 512],
            preferred_element_type=F32,
        )

    def down_for_mate(kx, half):
        for n in range(3):
            ps[kx, half, :, n * 512 : n * 512 + 512] = down(kx * 2 + 1, half, n).astype(BF16)
        send(ps.at[kx, half], pr.at[kx, half], pr_s.at[kx, half], pr_r.at[kx, half], mate)

    def down_mine(kx, half, dst):
        wait(pr.at[kx, half], pr_r.at[kx, half])
        for n in range(3):
            cols = slice(n * 512, n * 512 + 512)
            terms = down(kx * 2, half, n) + pr[kx, half, :, cols].astype(F32)
            dst[half * 256 : half * 256 + 256, cols] = terms.astype(BF16)

    def to_sides(p):
        for h, device in ((0, near), (1, far)):
            send(
                q1.at[pl.ds(base(h, p), 64), :],
                xr.at[h, pl.ds(p * 64, 64), :],
                xq_s.at[h],
                xq_r.at[h, p],
                device,
            )

    def home(h, p, src, first):
        for dy in range(4):
            at = pl.ds(p * 64 + dy * SLOTS, SLOTS)
            if p == 0 and dy == 0:
                rb[h, 0:SLOTS, :] = src[first : first + SLOTS, :]
                continue
            send(
                src.at[pl.ds(first + dy * SLOTS, SLOTS), :],
                rb.at[h, at, :],
                r2_s.at[h],
                r2_r.at[h, p],
                plane(-STEP[p] + 4, -dy + 4),
            )

    def wait_home(h):
        wait(rb.at[h, pl.ds(SLOTS, 48), :], r2_r.at[h, 0])
        for p in range(1, 4):
            wait(rb.at[h, pl.ds(p * 64, 64), :], r2_r.at[h, p])

    def combine(h, weight):
        high = weight.astype(BF16)
        rest = weight - high.astype(F32)
        middle = rest.astype(BF16)
        low = (rest - middle.astype(F32)).astype(BF16)
        stacked = jnp.concatenate([high, middle, low], axis=0)
        terms = jnp.dot(stacked, rb[h], preferred_element_type=F32)
        return terms[0:TOK] + terms[TOK : 2 * TOK] + terms[2 * TOK : 3 * TOK]

    weights(2, 3)
    down_for_mate(1, 1)
    down_for_mate(1, 0)
    weights(2, 2)
    down_mine(1, 1, q1)
    to_sides(3)
    to_sides(2)
    down_mine(1, 0, q1)
    to_sides(1)
    to_sides(0)
    weights(2, 1)
    down_for_mate(0, 1)
    down_for_mate(0, 0)
    weights(2, 0)
    down_mine(0, 1, q0)
    home(1, 3, q0, base(1, 3))
    home(1, 2, q0, base(1, 2))
    down_mine(0, 0, q0)
    home(1, 1, q0, base(1, 1))
    home(1, 0, q0, base(1, 0))

    for p in (3, 2, 1, 0):
        rows = slice(p * 64, p * 64 + 64)
        for h in range(2):
            wait(xr.at[h, pl.ds(p * 64, 64), :], xq_r.at[h, p])
        terms = q0[base(0, p) : base(0, p) + 64, :].astype(F32)
        terms = terms + xr[0, rows, :].astype(F32) + xr[1, rows, :].astype(F32)
        own[rows, :] = terms.astype(BF16)
        home(0, p, own, p * 64)
        if p == 1:
            wait_home(1)
            fin[0] = combine(1, weight_opp).astype(BF16)
            send(fin.at[0], fin.at[1], fin_s, fin_r, opp)

    wait_home(0)
    added = combine(0, weight_own)
    wait(fin.at[1], fin_r)
    out_ref[...] = (x_ref[...].astype(F32) + (added + fin[1].astype(F32))).astype(BF16)

    wait(sq.at[pl.ds(0, 3)], sq_s)
    wait(rt.at[0], rt_s)
    wait(nm.at[0], nm_s)
    for h in range(2):
        wait(pk.at[h, pl.ds(SLOTS, 240), :], s1_s.at[h])
        wait(xb.at[0, 0, pl.ds(0, 256), :], xf_s.at[h])
        wait(xb.at[h, 0], dd_s.at[h])
        for half in range(2):
            wait(ps.at[h, half], pr_s.at[h, half])
        wait(xr.at[h], xq_s.at[h])
        wait(rb.at[h, pl.ds(SLOTS, 240), :], r2_s.at[h])
    wait(fin.at[0], fin_s)


def on_device(
    queries,
    k_cache,
    v_cache,
    lengths,
    moe_input,
    norm_gain,
    expert_ids,
    combine_weights,
    capacity,
    w_gate,
    w_up,
    w_down,
):
    vmem = pl.BlockSpec(memory_space=pltpu.VMEM)
    smem = pl.BlockSpec(memory_space=pltpu.SMEM)
    hbm = pl.BlockSpec(memory_space=pl.ANY)
    dma = pltpu.SemaphoreType.DMA
    return pl.pallas_call(
        kernel,
        out_shape=(
            jax.ShapeDtypeStruct(queries.shape, BF16),
            jax.ShapeDtypeStruct(moe_input.shape, BF16),
        ),
        in_specs=[smem, smem, vmem, vmem, vmem, vmem, vmem, hbm, hbm, hbm, hbm, hbm],
        out_specs=(vmem, vmem),
        scratch_shapes=[
            pltpu.VMEM((SEQS, 2, 128, 128), BF16),
            pltpu.VMEM((SEQS, 2, 128, 128), BF16),
            pltpu.VMEM((4, FEAT, HID), BF16),
            pltpu.VMEM((4, FEAT, HID), BF16),
            pltpu.VMEM((4, HID, FEAT), BF16),
            pltpu.VMEM((2, 2, ROWS, FEAT), BF16),
            pltpu.VMEM((2, 256, FEAT), BF16),
            pltpu.VMEM((ROWS, HID), F32),
            pltpu.VMEM((ROWS, HID), F32),
            pltpu.VMEM((ROWS, HID), BF16),
            pltpu.VMEM((2, 2, 256, FEAT), BF16),
            pltpu.VMEM((2, 2, 256, FEAT), BF16),
            pltpu.VMEM((ROWS, FEAT), BF16),
            pltpu.VMEM((ROWS, FEAT), BF16),
            pltpu.VMEM((2, 256, FEAT), BF16),
            pltpu.VMEM((256, FEAT), BF16),
            pltpu.VMEM((2, 256, FEAT), BF16),
            pltpu.VMEM((4, TOK, 128), F32),
            pltpu.VMEM((2, TOK, 128), F32),
            pltpu.VMEM((2, TOK, FEAT), BF16),
            pltpu.VMEM((2, TOK, FEAT), BF16),
            dma((3, 4)),
            dma((2,)),
            dma,
            dma((4,)),
            dma,
            dma,
            dma,
            dma,
            dma((2,)),
            dma((2, 4)),
            dma((2,)),
            dma((2, 4)),
            dma((2,)),
            dma((2, 2)),
            dma((2, 2)),
            dma((2, 2)),
            dma((2,)),
            dma((2, 4)),
            dma((2,)),
            dma((2, 4)),
            dma,
            dma,
        ],
        compiler_params=pltpu.CompilerParams(
            collective_id=0, has_side_effects=True, vmem_limit_bytes=62 * 1024 * 1024
        ),
    )(
        lengths,
        capacity,
        queries,
        moe_input,
        norm_gain.reshape(1, FEAT),
        expert_ids,
        combine_weights,
        k_cache,
        v_cache,
        w_gate,
        w_up,
        w_down,
    )


def solution(mesh):
    in_specs = (
        P("expert", "mp", None),
        P("expert", "mp", None, None),
        P("expert", "mp", None, None),
        P("expert"),
        P("expert", "mp"),
        P("mp"),
        P("expert", None),
        P("expert", None),
        P(),
        P("expert", None, "mp"),
        P("expert", None, "mp"),
        P("expert", "mp", None),
    )
    out_specs = (P("expert", "mp", None), P("expert", "mp"))
    return jax.shard_map(
        on_device, mesh=mesh, in_specs=in_specs, out_specs=out_specs, check_vma=False
    )
```

```python
import jax
import jax.numpy as jnp
from jax import lax
from jax.experimental import pallas as pl
from jax.experimental.pallas import tpu as pltpu
from jax.sharding import PartitionSpec as P

MESH = pl.DeviceIdType.MESH
F32 = jnp.float32
BF16 = jnp.bfloat16

D = 6144
EXPERTS = 8
SLOTS = 16
TOK = 32
FEAT = 1536
HID = 512
ROWS = 512
SEQS = 32
STEP = (1, 2, 3, 0)


def base(h, p):
    return (p // 2) * 256 + h * 128 + (p % 2) * 64


def kernel(
    lengths,
    capacity,
    q_ref,
    x_ref,
    gain_ref,
    ids_ref,
    wts_ref,
    k_hbm,
    v_hbm,
    wg_hbm,
    wu_hbm,
    wd_hbm,
    ctx_ref,
    out_ref,
    kv,
    vv,
    wg,
    wu,
    wd,
    xb,
    pk,
    zb,
    yb,
    rz,
    acc_g,
    acc_u,
    hid,
    ps,
    pr,
    q1,
    q0,
    xr,
    own,
    rb,
    sq,
    rt,
    nm,
    fin,
    qf,
    cf,
    w_sem,
    kv_sem,
    sq_s,
    sq_r,
    rt_s,
    rt_r,
    nm_s,
    nm_r,
    s0_s,
    s0_r,
    s1_s,
    s1_r,
    xf_s,
    xf_r,
    dd_s,
    dd_r,
    pr_s,
    pr_r,
    xq_s,
    xq_r,
    r2_s,
    r2_r,
    r3_s,
    r3_r,
    fin_s,
    fin_r,
):
    s = lax.axis_index("expert")
    m = lax.axis_index("mp")
    z = s // 8
    y = (s // 2) % 4
    s_other = s + 1 - 2 * (s % 2)
    m_core = m + 1 - 2 * (m % 2)
    m_near = (m + 2) % 4
    m_both = 3 - m
    mates = (m, m_core, m_near, m_both)
    x_hi = s % 2
    mate = (s, m_core)
    near = (s, m_near)
    far = (s_other, m_near)
    opp = (s_other, m)

    def plane(dz, dy):
        return (((z + dz) % 4) * 8 + ((y + dy) % 4) * 2 + x_hi, m)

    def send(src, dst, send_sem, recv_sem, device):
        pltpu.make_async_remote_copy(
            src_ref=src,
            dst_ref=dst,
            send_sem=send_sem,
            recv_sem=recv_sem,
            device_id=device,
            device_id_type=MESH,
        ).start()

    def wait(ref, sem):
        pltpu.make_async_copy(ref, ref, sem).wait()

    copies = []
    for k in range(4):
        rows = pl.ds(pl.multiple_of(mates[k] * FEAT, FEAT), FEAT)
        copies.append(pltpu.make_async_copy(wg_hbm.at[0, rows, :], wg.at[k], w_sem.at[0, k]))
        copies.append(pltpu.make_async_copy(wu_hbm.at[0, rows, :], wu.at[k], w_sem.at[1, k]))
        copies.append(pltpu.make_async_copy(wd_hbm.at[0, :, rows], wd.at[k], w_sem.at[2, k]))
    k_copy = pltpu.make_async_copy(k_hbm, kv, kv_sem.at[0])
    v_copy = pltpu.make_async_copy(v_hbm, vv, kv_sem.at[1])
    k_copy.start()
    v_copy.start()
    for copy in copies:
        copy.start()

    barrier = pltpu.get_barrier_semaphore()
    partners = [plane(d, 0) for d in range(1, 4)] + [plane(0, d) for d in range(1, 4)]
    partners += [mate, near, far, opp, (s, m_both)]
    for device in partners:
        pl.semaphore_signal(barrier, inc=1, device_id=device, device_id_type=MESH)

    lane = lax.broadcasted_iota(jnp.int32, (TOK, 128), 1)
    across = lax.broadcasted_iota(jnp.int32, (TOK, TOK), 1)
    down_ward = lax.broadcasted_iota(jnp.int32, (TOK, TOK), 0)

    def column(row):
        return jnp.sum(jnp.where(across == down_ward, row, 0.0), axis=1, keepdims=True)

    ids = ids_ref[...].astype(F32)
    wts = wts_ref[...]
    route = jnp.where(
        lane == 0,
        column(ids[0:1]),
        jnp.where(
            lane == 1,
            column(ids[1:2]),
            jnp.where(lane == 2, column(wts[0:1]), column(wts[1:2])),
        ),
    )
    rt[0] = route
    x = x_ref[...].astype(F32)
    mine = jnp.sum(x * x, axis=1, keepdims=True)
    sq[0] = jnp.broadcast_to(mine, (TOK, 128))

    pl.semaphore_wait(barrier, len(partners))
    for k in range(1, 4):
        send(sq.at[0], sq.at[k], sq_s, sq_r.at[k], (s, mates[k]))
    send(rt.at[0], rt.at[1], rt_s, rt_r, opp)

    col = lax.broadcasted_iota(jnp.int32, (TOK, 128), 1)
    e_col = ((z + (col // 32 + 1) % 4) % 4) * 2 + (col // SLOTS) % 2
    j_col = col % SLOTS
    cap_col = jnp.zeros((TOK, 128), jnp.int32)
    for e in range(EXPERTS):
        cap_col = jnp.where(e_col == e, capacity[e], cap_col)
    open_col = j_col < cap_col
    e_col_f = e_col.astype(F32)
    j_col_f = j_col.astype(F32)
    tri = (across < down_ward).astype(F32).astype(BF16)

    def routing(route):
        first = route[:, 0:1] == e_col_f
        second = route[:, 1:2] == e_col_f
        member = first | second
        rank = jnp.dot(tri, member.astype(F32).astype(BF16), preferred_element_type=F32)
        take = member & (rank == j_col_f) & open_col
        weight = jnp.where(take, jnp.where(first, route[:, 2:3], route[:, 3:4]), 0.0)
        return take.astype(F32).astype(BF16), weight

    take_own, weight_own = routing(route)

    for k in range(1, 4):
        wait(sq.at[k], sq_r.at[k])
    total = (sq[0] + sq[1] + sq[2] + sq[3])[:, 0:1]
    normed = (x * lax.rsqrt(total / D + 1e-05) * gain_ref[...].reshape(1, FEAT)).astype(BF16)
    nm[0] = normed
    send(nm.at[0], nm.at[1], nm_s, nm_r, opp)

    def pack(h, take, features):
        packed = lax.dot_general(
            take, features, (((0,), (0,)), ((), ())), preferred_element_type=F32
        ).astype(BF16)
        pk[h] = packed
        zb[h, 96:128, :] = packed[96:128, :]
        for p in (0, 2, 1):
            rows = pl.ds(p * 32, 32)
            send(
                pk.at[h, rows, :], zb.at[h, rows, :], s0_s.at[h], s0_r.at[h, p], plane(STEP[p], 0)
            )

    def spread(h, p):
        if p != 3:
            wait(zb.at[h, pl.ds(p * 32, 32), :], s0_r.at[h, p])
        for dy in range(4):
            half = ((y + dy) % 4) // 2
            src = pl.ds(pl.multiple_of(p * 32 + half * SLOTS, SLOTS), SLOTS)
            at = base(h, p) + dy * SLOTS
            if dy == 0:
                xb[0, 0, at : at + SLOTS, :] = zb[h, src, :]
                continue
            send(
                zb.at[h, src, :],
                xb.at[0, 0, pl.ds(at, SLOTS), :],
                s1_s.at[h],
                s1_r.at[h, p],
                plane(0, dy),
            )

    def wait_slots(h, p):
        wait(xb.at[0, 0, pl.ds(base(h, p) + SLOTS, 48), :], s1_r.at[h, p])

    def to_mate(kx, h, p):
        rows = pl.ds(base(h, p), 64)
        send(xb.at[kx, 0, rows, :], xb.at[kx, 1, rows, :], dd_s.at[kx], dd_r.at[kx, p // 2], mate)

    def forward_own(p):
        wait_slots(0, p)
        rows = pl.ds(base(0, p), 64)
        send(xb.at[0, 0, rows, :], xb.at[1, 0, rows, :], xf_s.at[0], xf_r.at[0, p], near)
        send(
            xb.at[0, 0, rows, :],
            xb.at[1, 0, pl.ds(base(1, p), 64), :],
            xf_s.at[1],
            xf_r.at[1, p],
            far,
        )
        to_mate(0, 0, p)

    def forward_opp(p):
        wait_slots(1, p)
        to_mate(0, 1, p)

    def forward_side(p):
        for h in range(2):
            wait(xb.at[1, 0, pl.ds(base(h, p), 64), :], xf_r.at[h, p])
            to_mate(1, h, p)

    position = lax.broadcasted_iota(jnp.int32, (12, 256), 1)
    head = lax.broadcasted_iota(jnp.int32, (12, 128), 0)
    low_head = head < 6
    position = position[:, 0:128]

    def attend(b):
        scores = lax.dot_general(
            qf[pl.ds(b, 12, stride=SEQS), :].astype(BF16),
            kv[b].reshape(256, 128),
            (((1,), (1,)), ((), ())),
            preferred_element_type=F32,
        )
        scores = jnp.where(low_head, scores[:, 0:128], scores[:, 128:256]) * 128 ** (-0.5)
        scores = jnp.where(position < lengths[b], scores, -jnp.inf)
        expo = jnp.exp(scores - jnp.max(scores, axis=1, keepdims=True))
        probs = expo / jnp.sum(expo, axis=1, keepdims=True)
        both = jnp.concatenate(
            [jnp.where(low_head, probs, 0.0), jnp.where(low_head, 0.0, probs)], axis=1
        ).astype(BF16)
        cf[pl.ds(b, 12, stride=SEQS), :] = jnp.dot(
            both, vv[b].reshape(256, 128), preferred_element_type=F32
        )

    def attention(first, count):
        def some(i, carry):
            for u in range(8):
                attend(first + i * 8 + u)
            return carry

        lax.fori_loop(0, count // 8, some, 0)

    pack(0, take_own, normed)
    spread(0, 3)
    qf[...] = q_ref[...].astype(F32).reshape(12 * SEQS, 128)
    k_copy.wait()
    v_copy.wait()
    attention(0, 8)
    wait(rt.at[1], rt_r)
    take_opp, weight_opp = routing(rt[1])
    wait(nm.at[1], nm_r)
    pack(1, take_opp, nm[1])
    spread(0, 0)
    forward_own(3)
    spread(1, 3)
    attention(8, 8)
    spread(0, 1)
    forward_own(0)
    attention(16, 8)
    spread(1, 0)
    spread(0, 2)
    forward_side(3)
    spread(1, 1)
    forward_own(1)
    forward_opp(3)
    spread(1, 2)
    attention(24, 8)
    ctx_ref[...] = cf[...].reshape(12, SEQS, 128).astype(BF16)
    forward_opp(0)
    forward_side(0)
    forward_own(2)
    forward_opp(1)

    def gate_up(k, half):
        kx, cc = k // 2, k % 2
        rows = pl.ds(half * 256, 256)
        for n in range(2):
            cols = pl.ds(n * 256, 256)
            g = jnp.dot(xb[kx, cc, rows, :], wg[k, :, cols], preferred_element_type=F32)
            u = jnp.dot(xb[kx, cc, rows, :], wu[k, :, cols], preferred_element_type=F32)
            if k != 0:
                g = g + acc_g[rows, cols]
                u = u + acc_u[rows, cols]
            if k != 3:
                acc_g[rows, cols] = g
                acc_u[rows, cols] = u
            else:
                hid[rows, cols] = (g / (1.0 + jnp.exp(-g)) * u).astype(BF16)

    def weights(kind, k):
        copies[k * 3 + kind].wait()

    def down(k, half, n):
        return jnp.dot(
            hid[half * 256 : half * 256 + 256, :],
            wd[k, :, n * 512 : n * 512 + 512],
            preferred_element_type=F32,
        )

    def down_for_mate(kx, half):
        for n in range(3):
            ps[kx, half, :, n * 512 : n * 512 + 512] = down(kx * 2 + 1, half, n).astype(BF16)
        send(ps.at[kx, half], pr.at[kx, half], pr_s.at[kx, half], pr_r.at[kx, half], mate)

    def down_mine(kx, half, dst):
        wait(pr.at[kx, half], pr_r.at[kx, half])
        for n in range(3):
            cols = slice(n * 512, n * 512 + 512)
            terms = down(kx * 2, half, n) + pr[kx, half, :, cols].astype(F32)
            dst[half * 256 : half * 256 + 256, cols] = terms.astype(BF16)

    def to_sides(p):
        for h, device in ((0, near), (1, far)):
            send(
                q1.at[pl.ds(base(h, p), 64), :],
                xr.at[h, pl.ds(p * 64, 64), :],
                xq_s.at[h],
                xq_r.at[h, p],
                device,
            )

    def back_y(h, p, src, first):
        for dy in range(4):
            at = p * 64 + dy * SLOTS
            if dy == 0:
                yb[h, at : at + SLOTS, :] = src[first : first + SLOTS, :]
                continue
            send(
                src.at[pl.ds(first + dy * SLOTS, SLOTS), :],
                yb.at[h, pl.ds(at, SLOTS), :],
                r2_s.at[h],
                r2_r.at[h, p],
                plane(0, 4 - dy),
            )

    def back_z(h, p):
        wait(yb.at[h, pl.ds(p * 64 + SLOTS, 48), :], r2_r.at[h, p])
        for half in range(2):
            terms = jnp.zeros((SLOTS, FEAT), F32)
            for row in (2 * half, 2 * half + 1):
                at = p * 64 + ((row - y + 4) % 4) * SLOTS
                terms = terms + yb[h, pl.ds(pl.multiple_of(at, SLOTS), SLOTS), :].astype(F32)
            dst = rz if p != 3 else rb
            at = p * 32 + half * SLOTS
            dst[h, at : at + SLOTS, :] = terms.astype(BF16)
        if p != 3:
            rows = pl.ds(p * 32, 32)
            send(
                rz.at[h, rows, :], rb.at[h, rows, :], r3_s.at[h], r3_r.at[h], plane(4 - STEP[p], 0)
            )

    def wait_home(h):
        wait(rb.at[h, pl.ds(0, 96), :], r3_r.at[h])

    def combine(h, weight):
        high = weight.astype(BF16)
        rest = weight - high.astype(F32)
        middle = rest.astype(BF16)
        low = (rest - middle.astype(F32)).astype(BF16)
        stacked = jnp.concatenate([high, middle, low], axis=0)
        terms = jnp.dot(stacked, rb[h], preferred_element_type=F32)
        return terms[0:TOK] + terms[TOK : 2 * TOK] + terms[2 * TOK : 3 * TOK]

    def from_sides(p):
        rows = slice(p * 64, p * 64 + 64)
        for h in range(2):
            wait(xr.at[h, pl.ds(p * 64, 64), :], xq_r.at[h, p])
        terms = q0[base(0, p) : base(0, p) + 64, :].astype(F32)
        terms = terms + xr[0, rows, :].astype(F32) + xr[1, rows, :].astype(F32)
        own[rows, :] = terms.astype(BF16)
        back_y(0, p, own, p * 64)

    def from_mate(kx, half):
        wait(xb.at[kx, 1, pl.ds(half * 256, 256), :], dd_r.at[kx, half])

    for k in range(4):
        weights(0, k)
        weights(1, k)
    gate_up(0, 0)
    forward_side(1)
    from_mate(0, 0)
    gate_up(1, 0)
    gate_up(2, 0)
    forward_opp(2)
    from_mate(1, 0)
    gate_up(3, 0)
    for k in range(4):
        weights(2, k)
    down_for_mate(1, 0)
    gate_up(0, 1)
    from_mate(0, 1)
    gate_up(1, 1)
    down_mine(1, 0, q1)
    to_sides(0)
    to_sides(1)
    forward_side(2)
    down_for_mate(0, 0)
    gate_up(2, 1)
    down_mine(0, 0, q0)
    back_y(1, 0, q0, base(1, 0))
    back_y(1, 1, q0, base(1, 1))
    from_mate(1, 1)
    gate_up(3, 1)
    down_for_mate(1, 1)
    down_for_mate(0, 1)
    down_mine(1, 1, q1)
    to_sides(2)
    to_sides(3)
    down_mine(0, 1, q0)
    back_y(1, 2, q0, base(1, 2))
    back_y(1, 3, q0, base(1, 3))
    back_z(1, 0)
    from_sides(0)
    back_z(1, 1)
    from_sides(1)
    back_z(0, 0)
    back_z(1, 2)
    back_z(1, 3)
    from_sides(2)
    back_z(0, 1)
    wait_home(1)
    fin[0] = combine(1, weight_opp).astype(BF16)
    send(fin.at[0], fin.at[1], fin_s, fin_r, opp)
    back_z(0, 2)
    from_sides(3)
    back_z(0, 3)
    wait_home(0)
    added = combine(0, weight_own)
    wait(fin.at[1], fin_r)
    out_ref[...] = (x_ref[...].astype(F32) + (added + fin[1].astype(F32))).astype(BF16)

    wait(sq.at[pl.ds(0, 3)], sq_s)
    wait(rt.at[0], rt_s)
    wait(nm.at[0], nm_s)
    for h in range(2):
        wait(pk.at[h, pl.ds(0, 96), :], s0_s.at[h])
        wait(xb.at[0, 0, pl.ds(0, 192), :], s1_s.at[h])
        wait(xb.at[0, 0, pl.ds(0, 256), :], xf_s.at[h])
        wait(xb.at[h, 0], dd_s.at[h])
        for half in range(2):
            wait(ps.at[h, half], pr_s.at[h, half])
        wait(xr.at[h], xq_s.at[h])
        wait(yb.at[h, pl.ds(0, 192), :], r2_s.at[h])
        wait(rb.at[h, pl.ds(0, 96), :], r3_s.at[h])
    wait(fin.at[0], fin_s)


def on_device(
    queries,
    k_cache,
    v_cache,
    lengths,
    moe_input,
    norm_gain,
    expert_ids,
    combine_weights,
    capacity,
    w_gate,
    w_up,
    w_down,
):
    vmem = pl.BlockSpec(memory_space=pltpu.VMEM)
    smem = pl.BlockSpec(memory_space=pltpu.SMEM)
    hbm = pl.BlockSpec(memory_space=pl.ANY)
    dma = pltpu.SemaphoreType.DMA
    context, layer_out = pl.pallas_call(
        kernel,
        out_shape=(
            jax.ShapeDtypeStruct((12, SEQS, 128), BF16),
            jax.ShapeDtypeStruct(moe_input.shape, BF16),
        ),
        in_specs=[smem, smem, vmem, vmem, vmem, vmem, vmem, hbm, hbm, hbm, hbm, hbm],
        out_specs=(vmem, vmem),
        scratch_shapes=[
            pltpu.VMEM((SEQS, 2, 128, 128), BF16),
            pltpu.VMEM((SEQS, 2, 128, 128), BF16),
            pltpu.VMEM((4, FEAT, HID), BF16),
            pltpu.VMEM((4, FEAT, HID), BF16),
            pltpu.VMEM((4, HID, FEAT), BF16),
            pltpu.VMEM((2, 2, ROWS, FEAT), BF16),
            pltpu.VMEM((2, 128, FEAT), BF16),
            pltpu.VMEM((2, 128, FEAT), BF16),
            pltpu.VMEM((2, 256, FEAT), BF16),
            pltpu.VMEM((2, 128, FEAT), BF16),
            pltpu.VMEM((ROWS, HID), F32),
            pltpu.VMEM((ROWS, HID), F32),
            pltpu.VMEM((ROWS, HID), BF16),
            pltpu.VMEM((2, 2, 256, FEAT), BF16),
            pltpu.VMEM((2, 2, 256, FEAT), BF16),
            pltpu.VMEM((ROWS, FEAT), BF16),
            pltpu.VMEM((ROWS, FEAT), BF16),
            pltpu.VMEM((2, 256, FEAT), BF16),
            pltpu.VMEM((256, FEAT), BF16),
            pltpu.VMEM((2, 128, FEAT), BF16),
            pltpu.VMEM((4, TOK, 128), F32),
            pltpu.VMEM((2, TOK, 128), F32),
            pltpu.VMEM((2, TOK, FEAT), BF16),
            pltpu.VMEM((2, TOK, FEAT), BF16),
            pltpu.VMEM((12 * SEQS, 128), F32),
            pltpu.VMEM((12 * SEQS, 128), F32),
            dma((3, 4)),
            dma((2,)),
            dma,
            dma((4,)),
            dma,
            dma,
            dma,
            dma,
            dma((2,)),
            dma((2, 4)),
            dma((2,)),
            dma((2, 4)),
            dma((2,)),
            dma((2, 4)),
            dma((2,)),
            dma((2, 2)),
            dma((2, 2)),
            dma((2, 2)),
            dma((2,)),
            dma((2, 4)),
            dma((2,)),
            dma((2, 4)),
            dma((2,)),
            dma((2,)),
            dma,
            dma,
        ],
        compiler_params=pltpu.CompilerParams(
            collective_id=0, has_side_effects=True, vmem_limit_bytes=62 * 1024 * 1024
        ),
    )(
        lengths,
        capacity,
        queries.transpose(1, 0, 2),
        moe_input,
        norm_gain,
        expert_ids.T,
        combine_weights.T,
        k_cache,
        v_cache,
        w_gate,
        w_up,
        w_down,
    )
    return context.transpose(1, 0, 2), layer_out


def solution(mesh):
    in_specs = (
        P("expert", "mp", None),
        P("expert", "mp", None, None),
        P("expert", "mp", None, None),
        P("expert"),
        P("expert", "mp"),
        P("mp"),
        P("expert", None),
        P("expert", None),
        P(),
        P("expert", None, "mp"),
        P("expert", None, "mp"),
        P("expert", "mp", None),
    )
    out_specs = (P("expert", "mp", None), P("expert", "mp"))
    return jax.shard_map(
        on_device, mesh=mesh, in_specs=in_specs, out_specs=out_specs, check_vma=False
    )
```

```python
import jax
import jax.numpy as jnp
from jax import lax
from jax.experimental import pallas as pl
from jax.experimental.pallas import tpu as pltpu
from jax.sharding import PartitionSpec as P

MESH = pl.DeviceIdType.MESH
F32 = jnp.float32
BF16 = jnp.bfloat16

D = 6144
EXPERTS = 8
SLOTS = 16
TOK = 32
FEAT = 1536
HID = 512
ROWS = 512
SEQS = 32
STEP = (1, 2, 3, 0)


def base(h, p):
    return (p // 2) * 256 + h * 128 + (p % 2) * 64


def kernel(
    lengths,
    capacity,
    q_ref,
    x_ref,
    gain_ref,
    ids_ref,
    wts_ref,
    k_hbm,
    v_hbm,
    wg_hbm,
    wu_hbm,
    wd_hbm,
    ctx_ref,
    out_ref,
    kv,
    vv,
    wg,
    wu,
    wd,
    xb,
    pk,
    zb,
    yb,
    rz,
    acc_g,
    acc_u,
    hid,
    ps,
    pr,
    q1,
    q0,
    xr,
    own,
    rb,
    sq,
    rt,
    nm,
    fin,
    qf,
    cf,
    w_sem,
    kv_sem,
    sq_s,
    sq_r,
    rt_s,
    rt_r,
    nm_s,
    nm_r,
    s0_s,
    s0_r,
    s1_s,
    s1_r,
    xf_s,
    xf_r,
    dd_s,
    dd_r,
    pr_s,
    pr_r,
    xq_s,
    xq_r,
    r2_s,
    r2_r,
    r3_s,
    r3_r,
    fin_s,
    fin_r,
):
    s = lax.axis_index("expert")
    m = lax.axis_index("mp")
    z = s // 8
    y = (s // 2) % 4
    s_other = s + 1 - 2 * (s % 2)
    m_core = m + 1 - 2 * (m % 2)
    m_near = (m + 2) % 4
    m_both = 3 - m
    mates = (m, m_core, m_near, m_both)
    x_hi = s % 2
    mate = (s, m_core)
    near = (s, m_near)
    far = (s_other, m_near)
    opp = (s_other, m)

    def plane(dz, dy):
        return (((z + dz) % 4) * 8 + ((y + dy) % 4) * 2 + x_hi, m)

    def send(src, dst, send_sem, recv_sem, device):
        pltpu.make_async_remote_copy(
            src_ref=src,
            dst_ref=dst,
            send_sem=send_sem,
            recv_sem=recv_sem,
            device_id=device,
            device_id_type=MESH,
        ).start()

    def wait(ref, sem):
        pltpu.make_async_copy(ref, ref, sem).wait()

    barrier = pltpu.get_barrier_semaphore()
    partners = [plane(d, 0) for d in range(1, 4)] + [plane(0, d) for d in range(1, 4)]
    partners += [mate, near, far, opp, (s, m_both)]
    for device in partners:
        pl.semaphore_signal(barrier, inc=1, device_id=device, device_id_type=MESH)

    copies = []
    for k in range(4):
        rows = pl.ds(pl.multiple_of(mates[k] * FEAT, FEAT), FEAT)
        copies.append(pltpu.make_async_copy(wg_hbm.at[0, rows, :], wg.at[k], w_sem.at[0, k]))
        copies.append(pltpu.make_async_copy(wu_hbm.at[0, rows, :], wu.at[k], w_sem.at[1, k]))
        copies.append(pltpu.make_async_copy(wd_hbm.at[0, :, rows], wd.at[k], w_sem.at[2, k]))
    k_copy = pltpu.make_async_copy(k_hbm, kv, kv_sem.at[0])
    v_copy = pltpu.make_async_copy(v_hbm, vv, kv_sem.at[1])
    k_copy.start()
    v_copy.start()
    for copy in copies:
        copy.start()

    lane = lax.broadcasted_iota(jnp.int32, (TOK, 128), 1)
    across = lax.broadcasted_iota(jnp.int32, (TOK, TOK), 1)
    down_ward = lax.broadcasted_iota(jnp.int32, (TOK, TOK), 0)

    def column(row):
        return jnp.sum(jnp.where(across == down_ward, row, 0.0), axis=1, keepdims=True)

    ids = ids_ref[...].astype(F32)
    wts = wts_ref[...]
    route = jnp.where(
        lane == 0,
        column(ids[0:1]),
        jnp.where(
            lane == 1,
            column(ids[1:2]),
            jnp.where(lane == 2, column(wts[0:1]), column(wts[1:2])),
        ),
    )
    rt[0] = route
    x = x_ref[...].astype(F32)
    mine = jnp.sum(x * x, axis=1, keepdims=True)
    sq[0] = jnp.broadcast_to(mine, (TOK, 128))

    pl.semaphore_wait(barrier, len(partners))
    for k in range(1, 4):
        send(sq.at[0], sq.at[k], sq_s, sq_r.at[k], (s, mates[k]))
    send(rt.at[0], rt.at[1], rt_s, rt_r, opp)

    col = lax.broadcasted_iota(jnp.int32, (TOK, 128), 1)
    e_col = ((z + (col // 32 + 1) % 4) % 4) * 2 + (col // SLOTS) % 2
    j_col = col % SLOTS
    cap_col = jnp.zeros((TOK, 128), jnp.int32)
    for e in range(EXPERTS):
        cap_col = jnp.where(e_col == e, capacity[e], cap_col)
    open_col = j_col < cap_col
    e_col_f = e_col.astype(F32)
    j_col_f = j_col.astype(F32)
    tri = (across < down_ward).astype(F32).astype(BF16)

    def routing(route):
        first = route[:, 0:1] == e_col_f
        second = route[:, 1:2] == e_col_f
        member = first | second
        rank = jnp.dot(tri, member.astype(F32).astype(BF16), preferred_element_type=F32)
        take = member & (rank == j_col_f) & open_col
        weight = jnp.where(take, jnp.where(first, route[:, 2:3], route[:, 3:4]), 0.0)
        return take.astype(F32).astype(BF16), weight

    take_own, weight_own = routing(route)

    for k in range(1, 4):
        wait(sq.at[k], sq_r.at[k])
    total = (sq[0] + sq[1] + sq[2] + sq[3])[:, 0:1]
    normed = (x * lax.rsqrt(total / D + 1e-05) * gain_ref[...].reshape(1, FEAT)).astype(BF16)
    nm[0] = normed
    send(nm.at[0], nm.at[1], nm_s, nm_r, opp)

    def pack(h, take, features):
        packed = lax.dot_general(
            take, features, (((0,), (0,)), ((), ())), preferred_element_type=F32
        ).astype(BF16)
        pk[h] = packed
        zb[h, 96:128, :] = packed[96:128, :]
        for p in (0, 2, 1):
            rows = pl.ds(p * 32, 32)
            send(
                pk.at[h, rows, :], zb.at[h, rows, :], s0_s.at[h], s0_r.at[h, p], plane(STEP[p], 0)
            )

    def spread(h, p):
        if p != 3:
            wait(zb.at[h, pl.ds(p * 32, 32), :], s0_r.at[h, p])
        for dy in range(4):
            half = ((y + dy) % 4) // 2
            src = pl.ds(pl.multiple_of(p * 32 + half * SLOTS, SLOTS), SLOTS)
            at = base(h, p) + dy * SLOTS
            if dy == 0:
                xb[0, 0, at : at + SLOTS, :] = zb[h, src, :]
                continue
            send(
                zb.at[h, src, :],
                xb.at[0, 0, pl.ds(at, SLOTS), :],
                s1_s.at[h],
                s1_r.at[h, p],
                plane(0, dy),
            )

    def wait_slots(h, p):
        wait(xb.at[0, 0, pl.ds(base(h, p) + SLOTS, 48), :], s1_r.at[h, p])

    def to_mate(kx, h, p):
        rows = pl.ds(base(h, p), 64)
        send(xb.at[kx, 0, rows, :], xb.at[kx, 1, rows, :], dd_s.at[kx], dd_r.at[kx, p // 2], mate)

    def forward_own(p):
        wait_slots(0, p)
        rows = pl.ds(base(0, p), 64)
        send(xb.at[0, 0, rows, :], xb.at[1, 0, rows, :], xf_s.at[0], xf_r.at[0, p], near)
        send(
            xb.at[0, 0, rows, :],
            xb.at[1, 0, pl.ds(base(1, p), 64), :],
            xf_s.at[1],
            xf_r.at[1, p],
            far,
        )
        to_mate(0, 0, p)

    def forward_opp(p):
        wait_slots(1, p)
        to_mate(0, 1, p)

    def forward_side(p):
        for h in range(2):
            wait(xb.at[1, 0, pl.ds(base(h, p), 64), :], xf_r.at[h, p])
            to_mate(1, h, p)

    position = lax.broadcasted_iota(jnp.int32, (16, 128), 1)
    low_head = lax.broadcasted_iota(jnp.int32, (16, 128), 0) < 6
    nowhere = jnp.zeros((16, 128), BF16)

    def attention(first, count):
        scores = []
        for b in range(first, first + count):
            both = lax.dot_general(
                qf[pl.ds(b, 16, stride=SEQS), :].astype(BF16),
                kv[b].reshape(256, 128),
                (((1,), (1,)), ((), ())),
                preferred_element_type=F32,
            )
            both = jnp.where(low_head, both[:, 0:128], both[:, 128:256]) * 128 ** (-0.5)
            scores.append(jnp.where(position < lengths[b], both, -jnp.inf))
        scores = jnp.concatenate(scores, axis=0)
        expo = jnp.exp(scores - jnp.max(scores, axis=1, keepdims=True))
        probs = (expo / jnp.sum(expo, axis=1, keepdims=True)).astype(BF16)
        for u in range(count):
            mine = probs[u * 16 : u * 16 + 16]
            both = jnp.concatenate(
                [jnp.where(low_head, mine, nowhere), jnp.where(low_head, nowhere, mine)], axis=1
            )
            found = jnp.dot(both, vv[first + u].reshape(256, 128), preferred_element_type=F32)
            cf[pl.ds(first + u, 12, stride=SEQS), :] = found[0:12]

    pack(0, take_own, normed)
    spread(0, 3)
    qf[0 : 12 * SEQS, :] = q_ref[...].astype(F32).reshape(12 * SEQS, 128)
    qf[12 * SEQS : 16 * SEQS, :] = jnp.zeros((4 * SEQS, 128), F32)
    k_copy.wait()
    v_copy.wait()
    attention(0, 4)
    attention(4, 4)
    wait(rt.at[1], rt_r)
    take_opp, weight_opp = routing(rt[1])
    wait(nm.at[1], nm_r)
    pack(1, take_opp, nm[1])
    spread(0, 0)
    forward_own(3)
    attention(8, 4)
    spread(0, 1)
    spread(0, 2)
    attention(12, 4)
    forward_own(0)
    spread(1, 0)
    spread(1, 1)
    forward_own(1)
    spread(1, 3)
    spread(1, 2)
    forward_side(3)
    forward_own(2)
    attention(16, 4)
    forward_opp(0)
    forward_side(0)
    forward_opp(1)

    def gate_up(k, half):
        kx, cc = k // 2, k % 2
        rows = pl.ds(half * 256, 256)
        for n in range(2):
            cols = pl.ds(n * 256, 256)
            g = jnp.dot(xb[kx, cc, rows, :], wg[k, :, cols], preferred_element_type=F32)
            u = jnp.dot(xb[kx, cc, rows, :], wu[k, :, cols], preferred_element_type=F32)
            if k != 0:
                g = g + acc_g[rows, cols]
                u = u + acc_u[rows, cols]
            if k != 3:
                acc_g[rows, cols] = g
                acc_u[rows, cols] = u
            else:
                hid[rows, cols] = (g / (1.0 + jnp.exp(-g)) * u).astype(BF16)

    def weights(kind, k):
        copies[k * 3 + kind].wait()

    def down(k, half, n):
        return jnp.dot(
            hid[half * 256 : half * 256 + 256, :],
            wd[k, :, n * 512 : n * 512 + 512],
            preferred_element_type=F32,
        )

    def down_for_mate(kx, half):
        for n in range(3):
            ps[kx, half, :, n * 512 : n * 512 + 512] = down(kx * 2 + 1, half, n).astype(BF16)
        send(ps.at[kx, half], pr.at[kx, half], pr_s.at[kx, half], pr_r.at[kx, half], mate)

    def down_mine(kx, half, dst):
        wait(pr.at[kx, half], pr_r.at[kx, half])
        for n in range(3):
            cols = slice(n * 512, n * 512 + 512)
            terms = down(kx * 2, half, n) + pr[kx, half, :, cols].astype(F32)
            dst[half * 256 : half * 256 + 256, cols] = terms.astype(BF16)

    def to_sides(p):
        for h, device in ((0, near), (1, far)):
            send(
                q1.at[pl.ds(base(h, p), 64), :],
                xr.at[h, pl.ds(p * 64, 64), :],
                xq_s.at[h],
                xq_r.at[h, p],
                device,
            )

    def back_y(h, p, src, first):
        for dy in range(4):
            at = p * 64 + dy * SLOTS
            if dy == 0:
                yb[h, at : at + SLOTS, :] = src[first : first + SLOTS, :]
                continue
            send(
                src.at[pl.ds(first + dy * SLOTS, SLOTS), :],
                yb.at[h, pl.ds(at, SLOTS), :],
                r2_s.at[h],
                r2_r.at[h, p],
                plane(0, 4 - dy),
            )

    def back_z(h, p):
        wait(yb.at[h, pl.ds(p * 64 + SLOTS, 48), :], r2_r.at[h, p])
        for half in range(2):
            terms = jnp.zeros((SLOTS, FEAT), F32)
            for row in (2 * half, 2 * half + 1):
                at = p * 64 + ((row - y + 4) % 4) * SLOTS
                terms = terms + yb[h, pl.ds(pl.multiple_of(at, SLOTS), SLOTS), :].astype(F32)
            dst = rz if p != 3 else rb
            at = p * 32 + half * SLOTS
            dst[h, at : at + SLOTS, :] = terms.astype(BF16)
        if p != 3:
            rows = pl.ds(p * 32, 32)
            send(
                rz.at[h, rows, :], rb.at[h, rows, :], r3_s.at[h], r3_r.at[h], plane(4 - STEP[p], 0)
            )

    def wait_home(h):
        wait(rb.at[h, pl.ds(0, 96), :], r3_r.at[h])

    def combine(h, weight):
        high = weight.astype(BF16)
        rest = weight - high.astype(F32)
        middle = rest.astype(BF16)
        low = (rest - middle.astype(F32)).astype(BF16)
        stacked = jnp.concatenate([high, middle, low], axis=0)
        terms = jnp.dot(stacked, rb[h], preferred_element_type=F32)
        return terms[0:TOK] + terms[TOK : 2 * TOK] + terms[2 * TOK : 3 * TOK]

    def from_sides(p):
        rows = slice(p * 64, p * 64 + 64)
        for h in range(2):
            wait(xr.at[h, pl.ds(p * 64, 64), :], xq_r.at[h, p])
        terms = q0[base(0, p) : base(0, p) + 64, :].astype(F32)
        terms = terms + xr[0, rows, :].astype(F32) + xr[1, rows, :].astype(F32)
        own[rows, :] = terms.astype(BF16)
        back_y(0, p, own, p * 64)

    def from_mate(kx, half):
        wait(xb.at[kx, 1, pl.ds(half * 256, 256), :], dd_r.at[kx, half])

    for k in range(4):
        weights(0, k)
        weights(1, k)
    gate_up(0, 0)
    from_mate(0, 0)
    gate_up(1, 0)
    forward_opp(3)
    forward_side(1)
    gate_up(2, 0)
    from_mate(1, 0)
    gate_up(3, 0)
    forward_opp(2)
    for k in range(4):
        weights(2, k)
    down_for_mate(1, 0)
    gate_up(0, 1)
    forward_side(2)
    down_mine(1, 0, q1)
    to_sides(0)
    to_sides(1)
    from_mate(0, 1)
    gate_up(1, 1)
    down_for_mate(0, 0)
    gate_up(2, 1)
    from_mate(1, 1)
    gate_up(3, 1)
    down_for_mate(1, 1)
    down_mine(0, 0, q0)
    back_y(1, 0, q0, base(1, 0))
    back_y(1, 1, q0, base(1, 1))
    down_mine(1, 1, q1)
    to_sides(2)
    to_sides(3)
    from_sides(0)
    down_for_mate(0, 1)
    attention(20, 4)
    down_mine(0, 1, q0)
    back_y(1, 2, q0, base(1, 2))
    back_y(1, 3, q0, base(1, 3))
    back_z(1, 0)
    from_sides(1)
    attention(24, 4)
    back_z(1, 1)
    back_z(0, 0)
    attention(28, 4)
    ctx_ref[...] = cf[...].reshape(12, SEQS, 128).astype(BF16)
    from_sides(2)
    back_z(1, 2)
    back_z(1, 3)
    back_z(0, 1)
    from_sides(3)
    wait_home(1)
    fin[0] = combine(1, weight_opp).astype(BF16)
    send(fin.at[0], fin.at[1], fin_s, fin_r, opp)
    back_z(0, 2)
    back_z(0, 3)
    wait_home(0)
    added = combine(0, weight_own)
    wait(fin.at[1], fin_r)
    out_ref[...] = (x_ref[...].astype(F32) + (added + fin[1].astype(F32))).astype(BF16)

    wait(sq.at[pl.ds(0, 3)], sq_s)
    wait(rt.at[0], rt_s)
    wait(nm.at[0], nm_s)
    for h in range(2):
        wait(pk.at[h, pl.ds(0, 96), :], s0_s.at[h])
        wait(xb.at[0, 0, pl.ds(0, 192), :], s1_s.at[h])
        wait(xb.at[0, 0, pl.ds(0, 256), :], xf_s.at[h])
        wait(xb.at[h, 0], dd_s.at[h])
        for half in range(2):
            wait(ps.at[h, half], pr_s.at[h, half])
        wait(xr.at[h], xq_s.at[h])
        wait(yb.at[h, pl.ds(0, 192), :], r2_s.at[h])
        wait(rb.at[h, pl.ds(0, 96), :], r3_s.at[h])
    wait(fin.at[0], fin_s)


def hand_on(context_in, layer_in, context_out, layer_out):
    context_out[...] = context_in[...]
    layer_out[...] = layer_in[...]


def on_device(
    queries,
    k_cache,
    v_cache,
    lengths,
    moe_input,
    norm_gain,
    expert_ids,
    combine_weights,
    capacity,
    w_gate,
    w_up,
    w_down,
):
    vmem = pl.BlockSpec(memory_space=pltpu.VMEM)
    smem = pl.BlockSpec(memory_space=pltpu.SMEM)
    hbm = pl.BlockSpec(memory_space=pl.ANY)
    dma = pltpu.SemaphoreType.DMA
    context, layer_out = pl.pallas_call(
        kernel,
        out_shape=(
            jax.ShapeDtypeStruct((12, SEQS, 128), BF16),
            jax.ShapeDtypeStruct(moe_input.shape, BF16),
        ),
        in_specs=[smem, smem, vmem, vmem, vmem, vmem, vmem, hbm, hbm, hbm, hbm, hbm],
        out_specs=(vmem, vmem),
        scratch_shapes=[
            pltpu.VMEM((SEQS, 2, 128, 128), BF16),
            pltpu.VMEM((SEQS, 2, 128, 128), BF16),
            pltpu.VMEM((4, FEAT, HID), BF16),
            pltpu.VMEM((4, FEAT, HID), BF16),
            pltpu.VMEM((4, HID, FEAT), BF16),
            pltpu.VMEM((2, 2, ROWS, FEAT), BF16),
            pltpu.VMEM((2, 128, FEAT), BF16),
            pltpu.VMEM((2, 128, FEAT), BF16),
            pltpu.VMEM((2, 256, FEAT), BF16),
            pltpu.VMEM((2, 128, FEAT), BF16),
            pltpu.VMEM((ROWS, HID), F32),
            pltpu.VMEM((ROWS, HID), F32),
            pltpu.VMEM((ROWS, HID), BF16),
            pltpu.VMEM((2, 2, 256, FEAT), BF16),
            pltpu.VMEM((2, 2, 256, FEAT), BF16),
            pltpu.VMEM((ROWS, FEAT), BF16),
            pltpu.VMEM((ROWS, FEAT), BF16),
            pltpu.VMEM((2, 256, FEAT), BF16),
            pltpu.VMEM((256, FEAT), BF16),
            pltpu.VMEM((2, 128, FEAT), BF16),
            pltpu.VMEM((4, TOK, 128), F32),
            pltpu.VMEM((2, TOK, 128), F32),
            pltpu.VMEM((2, TOK, FEAT), BF16),
            pltpu.VMEM((2, TOK, FEAT), BF16),
            pltpu.VMEM((16 * SEQS, 128), F32),
            pltpu.VMEM((12 * SEQS, 128), F32),
            dma((3, 4)),
            dma((2,)),
            dma,
            dma((4,)),
            dma,
            dma,
            dma,
            dma,
            dma((2,)),
            dma((2, 4)),
            dma((2,)),
            dma((2, 4)),
            dma((2,)),
            dma((2, 4)),
            dma((2,)),
            dma((2, 2)),
            dma((2, 2)),
            dma((2, 2)),
            dma((2,)),
            dma((2, 4)),
            dma((2,)),
            dma((2, 4)),
            dma((2,)),
            dma((2,)),
            dma,
            dma,
        ],
        compiler_params=pltpu.CompilerParams(
            collective_id=0, has_side_effects=True, vmem_limit_bytes=62 * 1024 * 1024
        ),
    )(
        lengths,
        capacity,
        queries.transpose(1, 0, 2),
        moe_input,
        norm_gain,
        expert_ids.T,
        combine_weights.T,
        k_cache,
        v_cache,
        w_gate,
        w_up,
        w_down,
    )
    context, layer_out = pl.pallas_call(
        hand_on,
        out_shape=(
            jax.ShapeDtypeStruct(context.shape, BF16),
            jax.ShapeDtypeStruct(layer_out.shape, BF16),
        ),
        in_specs=[vmem, vmem],
        out_specs=(vmem, vmem),
    )(context, layer_out)
    return context.transpose(1, 0, 2), layer_out


def solution(mesh):
    in_specs = (
        P("expert", "mp", None),
        P("expert", "mp", None, None),
        P("expert", "mp", None, None),
        P("expert"),
        P("expert", "mp"),
        P("mp"),
        P("expert", None),
        P("expert", None),
        P(),
        P("expert", None, "mp"),
        P("expert", None, "mp"),
        P("expert", "mp", None),
    )
    out_specs = (P("expert", "mp", None), P("expert", "mp"))
    return jax.shard_map(
        on_device, mesh=mesh, in_specs=in_specs, out_specs=out_specs, check_vma=False
    )
```

```python
import jax
import jax.numpy as jnp
from jax import lax
from jax.experimental import pallas as pl
from jax.experimental.pallas import tpu as pltpu
from jax.sharding import PartitionSpec as P

MESH = pl.DeviceIdType.MESH
F32 = jnp.float32
BF16 = jnp.bfloat16

D = 6144
EXPERTS = 8
SLOTS = 16
TOK = 32
FEAT = 1536
HID = 512
ROWS = 512
SEQS = 32
STEP = (1, 2, 3, 0)


def base(h, p):
    place = (p + 1) % 4
    return (place // 2) * 256 + h * 128 + (place % 2) * 64


def kernel(
    lengths,
    capacity,
    q_ref,
    x_ref,
    gain_ref,
    ids_ref,
    wts_ref,
    k_hbm,
    v_hbm,
    wg_hbm,
    wu_hbm,
    wd_hbm,
    ctx_ref,
    out_ref,
    kv,
    vv,
    wg,
    wu,
    wd,
    xb,
    pk,
    zb,
    yb,
    rz,
    acc_g,
    acc_u,
    hid,
    ps,
    pr,
    q1,
    q0,
    xr,
    own,
    rb,
    rd,
    sq,
    rt,
    raw,
    rs,
    fin,
    qf,
    cf,
    w_sem,
    kv_sem,
    sq_s,
    sq_r,
    rt_s,
    rt_r,
    raw_s,
    raw_r,
    rs_s,
    rs_r,
    s0_s,
    s0_r,
    s1_s,
    s1_r,
    xf_s,
    xf_r,
    dd_s,
    dd_r,
    pr_s,
    pr_r,
    xq_s,
    xq_r,
    r2_s,
    r2_r,
    r3_s,
    r3_r,
    rd_s,
    rd_r,
    fin_s,
    fin_r,
):
    s = lax.axis_index("expert")
    m = lax.axis_index("mp")
    z = s // 8
    y = (s // 2) % 4
    s_other = s + 1 - 2 * (s % 2)
    m_core = m + 1 - 2 * (m % 2)
    m_near = (m + 2) % 4
    m_both = 3 - m
    mates = (m, m_core, m_near, m_both)
    x_hi = s % 2
    mate = (s, m_core)
    near = (s, m_near)
    far = (s_other, m_near)
    opp = (s_other, m)

    def plane(dz, dy):
        return (((z + dz) % 4) * 8 + ((y + dy) % 4) * 2 + x_hi, m)

    def send(src, dst, send_sem, recv_sem, device):
        pltpu.make_async_remote_copy(
            src_ref=src,
            dst_ref=dst,
            send_sem=send_sem,
            recv_sem=recv_sem,
            device_id=device,
            device_id_type=MESH,
        ).start()

    def wait(ref, sem):
        pltpu.make_async_copy(ref, ref, sem).wait()

    barrier = pltpu.get_barrier_semaphore()
    partners = [plane(2, 0)]
    partners += [plane(dz, dy) for dz in (0, 1, 3) for dy in range(4) if (dz, dy) != (0, 0)]
    partners += [mate, near, far, opp, (s, m_both)]
    for device in partners:
        pl.semaphore_signal(barrier, inc=1, device_id=device, device_id_type=MESH)

    copies = []
    for k in range(4):
        rows = pl.ds(pl.multiple_of(mates[k] * FEAT, FEAT), FEAT)
        copies.append(pltpu.make_async_copy(wg_hbm.at[0, rows, :], wg.at[k], w_sem.at[0, k]))
        copies.append(pltpu.make_async_copy(wu_hbm.at[0, rows, :], wu.at[k], w_sem.at[1, k]))
        copies.append(pltpu.make_async_copy(wd_hbm.at[0, :, rows], wd.at[k], w_sem.at[2, k]))
    k_copy = pltpu.make_async_copy(k_hbm, kv, kv_sem.at[0])
    v_copy = pltpu.make_async_copy(v_hbm, vv, kv_sem.at[1])
    k_copy.start()
    v_copy.start()
    for copy in copies:
        copy.start()

    lane = lax.broadcasted_iota(jnp.int32, (TOK, 128), 1)
    across = lax.broadcasted_iota(jnp.int32, (TOK, TOK), 1)
    down_ward = lax.broadcasted_iota(jnp.int32, (TOK, TOK), 0)

    def column(row):
        return jnp.sum(jnp.where(across == down_ward, row, 0.0), axis=1, keepdims=True)

    ids = ids_ref[...].astype(F32)
    wts = wts_ref[...]
    route = jnp.where(
        lane == 0,
        column(ids[0:1]),
        jnp.where(
            lane == 1,
            column(ids[1:2]),
            jnp.where(lane == 2, column(wts[0:1]), column(wts[1:2])),
        ),
    )
    rt[0] = route
    x = x_ref[...].astype(F32)
    mine = jnp.sum(x * x, axis=1, keepdims=True)
    sq[0] = jnp.broadcast_to(mine, (TOK, 128))

    pl.semaphore_wait(barrier, len(partners))
    for k in range(1, 4):
        send(sq.at[0], sq.at[k], sq_s, sq_r.at[k], (s, mates[k]))
    send(rt.at[0], rt.at[1], rt_s, rt_r, opp)
    send(x_ref, raw, raw_s, raw_r, opp)

    col = lax.broadcasted_iota(jnp.int32, (TOK, 128), 1)
    e_col = ((z + (col // 32 + 1) % 4) % 4) * 2 + (col // SLOTS) % 2
    last = lax.broadcasted_iota(jnp.int32, (TOK, 64), 1)
    e_last = ((z + STEP[2]) % 4) * 2 + ((y + last // SLOTS) % 4) // 2

    tri = (across < down_ward).astype(F32).astype(BF16)

    def routing(route, e_col, j_col):
        cap_col = jnp.zeros(e_col.shape, jnp.int32)
        for e in range(EXPERTS):
            cap_col = jnp.where(e_col == e, capacity[e], cap_col)
        e_col = e_col.astype(F32)
        first = route[:, 0:1] == e_col
        second = route[:, 1:2] == e_col
        member = first | second
        rank = jnp.dot(tri, member.astype(F32).astype(BF16), preferred_element_type=F32)
        take = member & (rank == j_col.astype(F32)) & (j_col < cap_col)
        weight = jnp.where(take, jnp.where(first, route[:, 2:3], route[:, 3:4]), 0.0)
        return take.astype(F32).astype(BF16), weight

    take_own, weight_own = routing(route, e_col, col % SLOTS)

    for k in range(1, 4):
        wait(sq.at[k], sq_r.at[k])
    total = (sq[0] + sq[1] + sq[2] + sq[3])[:, 0:1]
    scale = lax.rsqrt(total / D + 1e-05)
    rs[0] = jnp.broadcast_to(scale, (TOK, 128))
    send(rs.at[0], rs.at[1], rs_s, rs_r, opp)
    gain = gain_ref[...].reshape(1, FEAT)

    def normed(tokens, scale):
        return (tokens.astype(F32) * scale * gain).astype(BF16)

    def pack(h, take, features):
        packed = lax.dot_general(
            take, features, (((0,), (0,)), ((), ())), preferred_element_type=F32
        ).astype(BF16)
        pk[h] = packed
        zb[h, 96:128, :] = packed[96:128, :]
        for p in (0, 2, 1):
            rows = pl.ds(p * 32, 32)
            send(
                pk.at[h, rows, :], zb.at[h, rows, :], s0_s.at[h], s0_r.at[h, p], plane(STEP[p], 0)
            )

    def spread(h, p):
        if p != 3:
            wait(zb.at[h, pl.ds(p * 32, 32), :], s0_r.at[h, p])
        for dy in range(4):
            half = ((y + dy) % 4) // 2
            src = pl.ds(pl.multiple_of(p * 32 + half * SLOTS, SLOTS), SLOTS)
            at = base(h, p) + dy * SLOTS
            if dy == 0:
                xb[0, 0, at : at + SLOTS, :] = zb[h, src, :]
                continue
            send(
                zb.at[h, src, :],
                xb.at[0, 0, pl.ds(at, SLOTS), :],
                s1_s.at[h],
                s1_r.at[h, p],
                plane(0, dy),
            )

    def wait_slots(h, p):
        wait(xb.at[0, 0, pl.ds(base(h, p) + SLOTS, 48), :], s1_r.at[h, p])

    def to_mate(kx, h, p):
        rows = pl.ds(base(h, p), 64)
        send(xb.at[kx, 0, rows, :], xb.at[kx, 1, rows, :], dd_s.at[kx], dd_r.at[kx, (p + 1) % 4 // 2], mate)

    def cross(p, skip, count):
        rows = pl.ds(base(0, p) + skip, count)
        send(xb.at[0, 0, rows, :], xb.at[1, 0, rows, :], xf_s.at[0], xf_r.at[0, p], near)
        send(
            xb.at[0, 0, rows, :],
            xb.at[1, 0, pl.ds(base(1, p) + skip, count), :],
            xf_s.at[1],
            xf_r.at[1, p],
            far,
        )

    def forward_own(p):
        wait_slots(0, p)
        cross(p, SLOTS, 48)
        to_mate(0, 0, p)

    def forward_opp(p):
        wait_slots(1, p)
        to_mate(0, 1, p)

    def forward_side(p):
        for h in range(2):
            wait(xb.at[1, 0, pl.ds(base(h, p), 64), :], xf_r.at[h, p])
            to_mate(1, h, p)

    position = lax.broadcasted_iota(jnp.int32, (16, 128), 1)
    low_head = lax.broadcasted_iota(jnp.int32, (16, 128), 0) < 6
    nowhere = jnp.zeros((16, 128), BF16)

    def attention(first, count):
        scores = []
        for b in range(first, first + count):
            both = lax.dot_general(
                qf[pl.ds(b, 16, stride=SEQS), :].astype(BF16),
                kv[b].reshape(256, 128),
                (((1,), (1,)), ((), ())),
                preferred_element_type=F32,
            )
            both = jnp.where(low_head, both[:, 0:128], both[:, 128:256]) * 128 ** (-0.5)
            scores.append(jnp.where(position < lengths[b], both, -jnp.inf))
        scores = jnp.concatenate(scores, axis=0)
        expo = jnp.exp(scores - jnp.max(scores, axis=1, keepdims=True))
        probs = (expo / jnp.sum(expo, axis=1, keepdims=True)).astype(BF16)
        for u in range(count):
            mine = probs[u * 16 : u * 16 + 16]
            both = jnp.concatenate(
                [jnp.where(low_head, mine, nowhere), jnp.where(low_head, nowhere, mine)], axis=1
            )
            found = jnp.dot(both, vv[first + u].reshape(256, 128), preferred_element_type=F32)
            cf[pl.ds(first + u, 12, stride=SEQS), :] = found[0:12]

    pack(0, take_own, normed(x, scale))
    spread(0, 3)
    cross(3, 0, SLOTS)
    qf[0 : 12 * SEQS, :] = q_ref[...].astype(F32).reshape(12 * SEQS, 128)
    qf[12 * SEQS : 16 * SEQS, :] = jnp.zeros((4 * SEQS, 128), F32)
    k_copy.wait()
    v_copy.wait()
    attention(0, 4)
    weight_last = routing(route, e_last, last % SLOTS)[1]
    weight_rest = jnp.where(col // 32 == 2, 0.0, weight_own)
    rb[0, 64:96, :] = jnp.zeros((32, FEAT), BF16)
    wait(rt.at[1], rt_r)
    take_opp, weight_opp = routing(rt[1], e_col, col % SLOTS)
    attention(4, 4)
    wait(raw, raw_r)
    wait(rs.at[1], rs_r)
    pack(1, take_opp, normed(raw[...], rs[1][:, 0:1]))
    spread(0, 0)
    cross(0, 0, SLOTS)
    forward_own(3)
    attention(8, 4)
    spread(1, 3)
    spread(0, 1)
    cross(1, 0, SLOTS)
    attention(12, 4)
    forward_own(0)
    spread(1, 0)
    spread(0, 2)
    cross(2, 0, SLOTS)
    spread(1, 1)
    spread(1, 2)
    attention(16, 4)
    forward_own(1)
    forward_opp(3)
    forward_side(3)
    forward_opp(0)

    def gate_up(k, half):
        kx, cc = k // 2, k % 2
        rows = pl.ds(half * 256, 256)
        for n in range(2):
            cols = pl.ds(n * 256, 256)
            g = jnp.dot(xb[kx, cc, rows, :], wg[k, :, cols], preferred_element_type=F32)
            u = jnp.dot(xb[kx, cc, rows, :], wu[k, :, cols], preferred_element_type=F32)
            if k != 0:
                g = g + acc_g[rows, cols]
                u = u + acc_u[rows, cols]
            if k != 3:
                acc_g[rows, cols] = g
                acc_u[rows, cols] = u
            else:
                hid[rows, cols] = (g / (1.0 + jnp.exp(-g)) * u).astype(BF16)

    def weights(kind, k):
        copies[k * 3 + kind].wait()

    def down(k, half, n):
        return jnp.dot(
            hid[half * 256 : half * 256 + 256, :],
            wd[k, :, n * 512 : n * 512 + 512],
            preferred_element_type=F32,
        )

    def down_for_mate(kx, half):
        for n in range(3):
            ps[kx, half, :, n * 512 : n * 512 + 512] = down(kx * 2 + 1, half, n).astype(BF16)
        send(ps.at[kx, half], pr.at[kx, half], pr_s.at[kx, half], pr_r.at[kx, half], mate)

    def down_mine(kx, half, dst):
        wait(pr.at[kx, half], pr_r.at[kx, half])
        for n in range(3):
            cols = slice(n * 512, n * 512 + 512)
            terms = down(kx * 2, half, n) + pr[kx, half, :, cols].astype(F32)
            dst[half * 256 : half * 256 + 256, cols] = terms.astype(BF16)

    def to_sides(p):
        for h, device in ((0, near), (1, far)):
            send(
                q1.at[pl.ds(base(h, p), 64), :],
                xr.at[h, pl.ds(p * 64, 64), :],
                xq_s.at[h],
                xq_r.at[h, p],
                device,
            )

    def back_y(h, p, src, first):
        for dy in range(4):
            at = p * 64 + dy * SLOTS
            if dy == 0:
                yb[h, at : at + SLOTS, :] = src[first : first + SLOTS, :]
                continue
            send(
                src.at[pl.ds(first + dy * SLOTS, SLOTS), :],
                yb.at[h, pl.ds(at, SLOTS), :],
                r2_s.at[h],
                r2_r.at[h, p],
                plane(0, 4 - dy),
            )

    def back_z(h, p):
        wait(yb.at[h, pl.ds(p * 64 + SLOTS, 48), :], r2_r.at[h, p])
        for half in range(2):
            terms = jnp.zeros((SLOTS, FEAT), F32)
            for row in (2 * half, 2 * half + 1):
                at = p * 64 + ((row - y + 4) % 4) * SLOTS
                terms = terms + yb[h, pl.ds(pl.multiple_of(at, SLOTS), SLOTS), :].astype(F32)
            dst = rz if p != 3 else rb
            at = p * 32 + half * SLOTS
            dst[h, at : at + SLOTS, :] = terms.astype(BF16)
        if p != 3:
            rows = pl.ds(p * 32, 32)
            send(
                rz.at[h, rows, :], rb.at[h, rows, :], r3_s.at[h], r3_r.at[h], plane(4 - STEP[p], 0)
            )

    def direct(p, src, first):
        for dy in range(4):
            rows = pl.ds(dy * SLOTS, SLOTS)
            send(
                src.at[pl.ds(first + dy * SLOTS, SLOTS), :],
                rd.at[rows, :],
                rd_s,
                rd_r,
                plane(4 - STEP[p], 4 - dy),
            )

    def combine(src, weight):
        high = weight.astype(BF16)
        rest = weight - high.astype(F32)
        middle = rest.astype(BF16)
        low = (rest - middle.astype(F32)).astype(BF16)
        stacked = jnp.concatenate([high, middle, low], axis=0)
        terms = jnp.dot(stacked, src, preferred_element_type=F32)
        return terms[0:TOK] + terms[TOK : 2 * TOK] + terms[2 * TOK : 3 * TOK]

    def from_sides(p):
        rows = slice(p * 64, p * 64 + 64)
        for h in range(2):
            wait(xr.at[h, pl.ds(p * 64, 64), :], xq_r.at[h, p])
        terms = q0[base(0, p) : base(0, p) + 64, :].astype(F32)
        terms = terms + xr[0, rows, :].astype(F32) + xr[1, rows, :].astype(F32)
        own[rows, :] = terms.astype(BF16)
        if p == 2:
            direct(p, own, p * 64)
        else:
            back_y(0, p, own, p * 64)

    def from_mate(kx, half):
        wait(xb.at[kx, 1, pl.ds(half * 256, 256), :], dd_r.at[kx, half])

    for k in range(4):
        weights(0, k)
        weights(1, k)
    gate_up(0, 0)
    forward_side(0)
    from_mate(0, 0)
    gate_up(1, 0)
    forward_own(2)
    gate_up(2, 0)
    from_mate(1, 0)
    gate_up(3, 0)
    forward_opp(1)
    for k in range(4):
        weights(2, k)
    down_for_mate(1, 0)
    down_for_mate(0, 0)
    forward_opp(2)
    gate_up(0, 1)
    forward_side(1)
    down_mine(1, 0, q1)
    to_sides(0)
    to_sides(3)
    down_mine(0, 0, q0)
    back_y(1, 0, q0, base(1, 0))
    back_y(1, 3, q0, base(1, 3))
    from_mate(0, 1)
    forward_side(2)
    gate_up(1, 1)
    gate_up(2, 1)
    from_mate(1, 1)
    gate_up(3, 1)
    down_for_mate(1, 1)
    down_for_mate(0, 1)
    attention(20, 4)
    down_mine(1, 1, q1)
    to_sides(1)
    to_sides(2)
    from_sides(0)
    down_mine(0, 1, q0)
    back_y(1, 1, q0, base(1, 1))
    back_y(1, 2, q0, base(1, 2))
    back_z(1, 0)
    back_z(1, 3)
    from_sides(3)
    attention(24, 4)
    back_z(0, 0)
    back_z(1, 1)
    from_sides(1)
    back_z(1, 2)
    attention(28, 4)
    ctx_ref[...] = cf[...].reshape(12, SEQS, 128).astype(BF16)
    back_z(0, 1)
    from_sides(2)
    back_z(0, 3)
    wait(rb.at[1, pl.ds(0, 96), :], r3_r.at[1])
    fin[0] = combine(rb[1], weight_opp).astype(BF16)
    send(fin.at[0], fin.at[1], fin_s, fin_r, opp)
    wait(rb.at[0, pl.ds(0, 64), :], r3_r.at[0])
    added = combine(rb[0], weight_rest)
    wait(fin.at[1], fin_r)
    added = added + fin[1].astype(F32)
    wait(rd, rd_r)
    added = added + combine(rd[...], weight_last)
    out_ref[...] = (x_ref[...].astype(F32) + added).astype(BF16)

    wait(sq.at[pl.ds(0, 3)], sq_s)
    wait(rt.at[0], rt_s)
    wait(raw, raw_s)
    wait(rs.at[0], rs_s)
    for h in range(2):
        wait(pk.at[h, pl.ds(0, 96), :], s0_s.at[h])
        wait(xb.at[0, 0, pl.ds(0, 192), :], s1_s.at[h])
        wait(xb.at[0, 0, pl.ds(0, 256), :], xf_s.at[h])
        wait(xb.at[h, 0], dd_s.at[h])
        for half in range(2):
            wait(ps.at[h, half], pr_s.at[h, half])
        wait(xr.at[h], xq_s.at[h])
        wait(yb.at[h, pl.ds(0, 144 + 48 * h), :], r2_s.at[h])
        wait(rb.at[h, pl.ds(0, 64 + 32 * h), :], r3_s.at[h])
    wait(rd, rd_s)
    wait(fin.at[0], fin_s)


def hand_on(context_in, layer_in, context_out, layer_out):
    context_out[...] = context_in[...]
    layer_out[...] = layer_in[...]


def on_device(
    queries,
    k_cache,
    v_cache,
    lengths,
    moe_input,
    norm_gain,
    expert_ids,
    combine_weights,
    capacity,
    w_gate,
    w_up,
    w_down,
):
    vmem = pl.BlockSpec(memory_space=pltpu.VMEM)
    smem = pl.BlockSpec(memory_space=pltpu.SMEM)
    hbm = pl.BlockSpec(memory_space=pl.ANY)
    dma = pltpu.SemaphoreType.DMA
    context, layer_out = pl.pallas_call(
        kernel,
        out_shape=(
            jax.ShapeDtypeStruct((12, SEQS, 128), BF16),
            jax.ShapeDtypeStruct(moe_input.shape, BF16),
        ),
        in_specs=[smem, smem, vmem, vmem, vmem, vmem, vmem, hbm, hbm, hbm, hbm, hbm],
        out_specs=(vmem, vmem),
        scratch_shapes=[
            pltpu.VMEM((SEQS, 2, 128, 128), BF16),
            pltpu.VMEM((SEQS, 2, 128, 128), BF16),
            pltpu.VMEM((4, FEAT, HID), BF16),
            pltpu.VMEM((4, FEAT, HID), BF16),
            pltpu.VMEM((4, HID, FEAT), BF16),
            pltpu.VMEM((2, 2, ROWS, FEAT), BF16),
            pltpu.VMEM((2, 128, FEAT), BF16),
            pltpu.VMEM((2, 128, FEAT), BF16),
            pltpu.VMEM((2, 256, FEAT), BF16),
            pltpu.VMEM((2, 128, FEAT), BF16),
            pltpu.VMEM((ROWS, HID), F32),
            pltpu.VMEM((ROWS, HID), F32),
            pltpu.VMEM((ROWS, HID), BF16),
            pltpu.VMEM((2, 2, 256, FEAT), BF16),
            pltpu.VMEM((2, 2, 256, FEAT), BF16),
            pltpu.VMEM((ROWS, FEAT), BF16),
            pltpu.VMEM((ROWS, FEAT), BF16),
            pltpu.VMEM((2, 256, FEAT), BF16),
            pltpu.VMEM((256, FEAT), BF16),
            pltpu.VMEM((2, 128, FEAT), BF16),
            pltpu.VMEM((64, FEAT), BF16),
            pltpu.VMEM((4, TOK, 128), F32),
            pltpu.VMEM((2, TOK, 128), F32),
            pltpu.VMEM((TOK, FEAT), BF16),
            pltpu.VMEM((2, TOK, 128), F32),
            pltpu.VMEM((2, TOK, FEAT), BF16),
            pltpu.VMEM((16 * SEQS, 128), F32),
            pltpu.VMEM((12 * SEQS, 128), F32),
            dma((3, 4)),
            dma((2,)),
            dma,
            dma((4,)),
            dma,
            dma,
            dma,
            dma,
            dma,
            dma,
            dma((2,)),
            dma((2, 4)),
            dma((2,)),
            dma((2, 4)),
            dma((2,)),
            dma((2, 4)),
            dma((2,)),
            dma((2, 2)),
            dma((2, 2)),
            dma((2, 2)),
            dma((2,)),
            dma((2, 4)),
            dma((2,)),
            dma((2, 4)),
            dma((2,)),
            dma((2,)),
            dma,
            dma,
            dma,
            dma,
        ],
        compiler_params=pltpu.CompilerParams(
            collective_id=0, has_side_effects=True, vmem_limit_bytes=62 * 1024 * 1024
        ),
    )(
        lengths,
        capacity,
        queries.transpose(1, 0, 2),
        moe_input,
        norm_gain,
        expert_ids.T,
        combine_weights.T,
        k_cache,
        v_cache,
        w_gate,
        w_up,
        w_down,
    )
    context, layer_out = pl.pallas_call(
        hand_on,
        out_shape=(
            jax.ShapeDtypeStruct(context.shape, BF16),
            jax.ShapeDtypeStruct(layer_out.shape, BF16),
        ),
        in_specs=[vmem, vmem],
        out_specs=(vmem, vmem),
    )(context, layer_out)
    return context.transpose(1, 0, 2), layer_out


def solution(mesh):
    in_specs = (
        P("expert", "mp", None),
        P("expert", "mp", None, None),
        P("expert", "mp", None, None),
        P("expert"),
        P("expert", "mp"),
        P("mp"),
        P("expert", None),
        P("expert", None),
        P(),
        P("expert", None, "mp"),
        P("expert", None, "mp"),
        P("expert", "mp", None),
    )
    out_specs = (P("expert", "mp", None), P("expert", "mp"))
    return jax.shard_map(
        on_device, mesh=mesh, in_specs=in_specs, out_specs=out_specs, check_vma=False
    )
```

```python
import jax
import jax.numpy as jnp
from jax import lax
from jax.experimental import pallas as pl
from jax.experimental.pallas import tpu as pltpu
from jax.sharding import PartitionSpec as P

MESH = pl.DeviceIdType.MESH
F32 = jnp.float32
BF16 = jnp.bfloat16

D = 6144
EXPERTS = 8
SLOTS = 16
TOK = 32
FEAT = 1536
HID = 512
ROWS = 512
SEQS = 32
STEP = (1, 2, 3, 0)


def base(h, p):
    place = (p + 1) % 4
    return (place // 2) * 256 + h * 128 + (place % 2) * 64


def kernel(
    lengths,
    capacity,
    q_ref,
    x_ref,
    gain_ref,
    ids_ref,
    wts_ref,
    k_hbm,
    v_hbm,
    wg_hbm,
    wu_hbm,
    wd_hbm,
    ctx_ref,
    out_ref,
    kv,
    vv,
    wg,
    wu,
    wd,
    xb,
    pk,
    zb,
    yb,
    rz,
    acc_g,
    acc_u,
    hid,
    ps,
    pr,
    q1,
    q0,
    xr,
    own,
    rb,
    rd,
    sq,
    rt,
    raw,
    rs,
    fin,
    qf,
    cf,
    w_sem,
    kv_sem,
    sq_s,
    sq_r,
    rt_s,
    rt_r,
    raw_s,
    raw_r,
    rs_s,
    rs_r,
    s0_s,
    s0_r,
    s1_s,
    s1_r,
    xf_s,
    xf_r,
    dd_s,
    dd_r,
    pr_s,
    pr_r,
    xq_s,
    xq_r,
    r2_s,
    r2_r,
    r3_s,
    r3_r,
    rd_s,
    rd_r,
    fin_s,
    fin_r,
):
    s = lax.axis_index("expert")
    m = lax.axis_index("mp")
    z = s // 8
    y = (s // 2) % 4
    s_other = s + 1 - 2 * (s % 2)
    m_core = m + 1 - 2 * (m % 2)
    m_near = (m + 2) % 4
    m_both = 3 - m
    mates = (m, m_core, m_near, m_both)
    x_hi = s % 2
    mate = (s, m_core)
    near = (s, m_near)
    far = (s_other, m_near)
    opp = (s_other, m)

    def plane(dz, dy):
        return (((z + dz) % 4) * 8 + ((y + dy) % 4) * 2 + x_hi, m)

    def send(src, dst, send_sem, recv_sem, device):
        pltpu.make_async_remote_copy(
            src_ref=src,
            dst_ref=dst,
            send_sem=send_sem,
            recv_sem=recv_sem,
            device_id=device,
            device_id_type=MESH,
        ).start()

    def wait(ref, sem):
        pltpu.make_async_copy(ref, ref, sem).wait()

    barrier = pltpu.get_barrier_semaphore()
    partners = [plane(2, 0)]
    partners += [plane(dz, dy) for dz in (0, 1, 3) for dy in range(4) if (dz, dy) != (0, 0)]
    partners += [mate, near, far, opp, (s, m_both)]
    for device in partners:
        pl.semaphore_signal(barrier, inc=1, device_id=device, device_id_type=MESH)

    copies = []
    for k in range(4):
        rows = pl.ds(pl.multiple_of(mates[k] * FEAT, FEAT), FEAT)
        copies.append(pltpu.make_async_copy(wg_hbm.at[0, rows, :], wg.at[k], w_sem.at[0, k]))
        copies.append(pltpu.make_async_copy(wu_hbm.at[0, rows, :], wu.at[k], w_sem.at[1, k]))
        copies.append(pltpu.make_async_copy(wd_hbm.at[0, :, rows], wd.at[k], w_sem.at[2, k]))
    k_copy = pltpu.make_async_copy(k_hbm, kv, kv_sem.at[0])
    v_copy = pltpu.make_async_copy(v_hbm, vv, kv_sem.at[1])
    k_copy.start()
    v_copy.start()
    for copy in copies:
        copy.start()

    lane = lax.broadcasted_iota(jnp.int32, (TOK, 128), 1)
    across = lax.broadcasted_iota(jnp.int32, (TOK, TOK), 1)
    down_ward = lax.broadcasted_iota(jnp.int32, (TOK, TOK), 0)

    def column(row):
        return jnp.sum(jnp.where(across == down_ward, row, 0.0), axis=1, keepdims=True)

    ids = ids_ref[...].astype(F32)
    wts = wts_ref[...]
    route = jnp.where(
        lane == 0,
        column(ids[0:1]),
        jnp.where(
            lane == 1,
            column(ids[1:2]),
            jnp.where(lane == 2, column(wts[0:1]), column(wts[1:2])),
        ),
    )
    rt[0] = route
    x = x_ref[...].astype(F32)
    mine = jnp.sum(x * x, axis=1, keepdims=True)
    sq[0] = jnp.broadcast_to(mine, (TOK, 128))

    pl.semaphore_wait(barrier, len(partners))
    for k in range(1, 4):
        send(sq.at[0], sq.at[k], sq_s, sq_r.at[k], (s, mates[k]))
    send(rt.at[0], rt.at[1], rt_s, rt_r, opp)
    send(x_ref, raw, raw_s, raw_r, opp)

    col = lax.broadcasted_iota(jnp.int32, (TOK, 128), 1)
    e_col = ((z + (col // 32 + 1) % 4) % 4) * 2 + (col // SLOTS) % 2
    last = lax.broadcasted_iota(jnp.int32, (TOK, 64), 1)
    e_last = ((z + STEP[2]) % 4) * 2 + ((y + last // SLOTS) % 4) // 2

    tri = (across < down_ward).astype(F32).astype(BF16)

    def routing(route, e_col, j_col):
        cap_col = jnp.zeros(e_col.shape, jnp.int32)
        for e in range(EXPERTS):
            cap_col = jnp.where(e_col == e, capacity[e], cap_col)
        e_col = e_col.astype(F32)
        first = route[:, 0:1] == e_col
        second = route[:, 1:2] == e_col
        member = first | second
        rank = jnp.dot(tri, member.astype(F32).astype(BF16), preferred_element_type=F32)
        take = member & (rank == j_col.astype(F32)) & (j_col < cap_col)
        weight = jnp.where(take, jnp.where(first, route[:, 2:3], route[:, 3:4]), 0.0)
        return take.astype(F32).astype(BF16), weight

    take_own, weight_own = routing(route, e_col, col % SLOTS)

    for k in range(1, 4):
        wait(sq.at[k], sq_r.at[k])
    total = (sq[0] + sq[1] + sq[2] + sq[3])[:, 0:1]
    scale = lax.rsqrt(total / D + 1e-05)
    rs[0] = jnp.broadcast_to(scale, (TOK, 128))
    send(rs.at[0], rs.at[1], rs_s, rs_r, opp)
    gain = gain_ref[...].reshape(1, FEAT)

    def normed(tokens, scale):
        return (tokens.astype(F32) * scale * gain).astype(BF16)

    def pack(h, take, features):
        packed = lax.dot_general(
            take, features, (((0,), (0,)), ((), ())), preferred_element_type=F32
        ).astype(BF16)
        pk[h] = packed
        zb[h, 96:128, :] = packed[96:128, :]
        for p in (0, 2, 1):
            rows = pl.ds(p * 32, 32)
            send(
                pk.at[h, rows, :], zb.at[h, rows, :], s0_s.at[h], s0_r.at[h, p], plane(STEP[p], 0)
            )

    def spread(h, p):
        if p != 3:
            wait(zb.at[h, pl.ds(p * 32, 32), :], s0_r.at[h, p])
        for dy in range(4):
            half = ((y + dy) % 4) // 2
            src = pl.ds(pl.multiple_of(p * 32 + half * SLOTS, SLOTS), SLOTS)
            at = base(h, p) + dy * SLOTS
            if dy == 0:
                xb[0, 0, at : at + SLOTS, :] = zb[h, src, :]
                continue
            send(
                zb.at[h, src, :],
                xb.at[0, 0, pl.ds(at, SLOTS), :],
                s1_s.at[h],
                s1_r.at[h, p],
                plane(0, dy),
            )

    def wait_slots(h, p):
        wait(xb.at[0, 0, pl.ds(base(h, p) + SLOTS, 48), :], s1_r.at[h, p])

    def to_mate(kx, h, p):
        rows = pl.ds(base(h, p), 64)
        send(xb.at[kx, 0, rows, :], xb.at[kx, 1, rows, :], dd_s.at[kx], dd_r.at[kx, (p + 1) % 4 // 2], mate)

    def cross(p, skip, count):
        rows = pl.ds(base(0, p) + skip, count)
        send(xb.at[0, 0, rows, :], xb.at[1, 0, rows, :], xf_s.at[0], xf_r.at[0, p], near)
        send(
            xb.at[0, 0, rows, :],
            xb.at[1, 0, pl.ds(base(1, p) + skip, count), :],
            xf_s.at[1],
            xf_r.at[1, p],
            far,
        )

    def forward_own(p):
        wait_slots(0, p)
        cross(p, SLOTS, 48)
        to_mate(0, 0, p)

    def forward_opp(p):
        wait_slots(1, p)
        to_mate(0, 1, p)

    def forward_side(p):
        for h in range(2):
            wait(xb.at[1, 0, pl.ds(base(h, p), 64), :], xf_r.at[h, p])
            to_mate(1, h, p)

    position = lax.broadcasted_iota(jnp.int32, (16, 128), 1)
    low_head = lax.broadcasted_iota(jnp.int32, (16, 128), 0) < 6
    nowhere = jnp.zeros((16, 128), BF16)

    def attention(first, count):
        scores = []
        for b in range(first, first + count):
            both = lax.dot_general(
                qf[pl.ds(b, 16, stride=SEQS), :].astype(BF16),
                kv[b].reshape(256, 128),
                (((1,), (1,)), ((), ())),
                preferred_element_type=F32,
            )
            both = jnp.where(low_head, both[:, 0:128], both[:, 128:256]) * 128 ** (-0.5)
            scores.append(jnp.where(position < lengths[b], both, -jnp.inf))
        scores = jnp.concatenate(scores, axis=0)
        expo = jnp.exp(scores - jnp.max(scores, axis=1, keepdims=True))
        probs = (expo / jnp.sum(expo, axis=1, keepdims=True)).astype(BF16)
        for u in range(count):
            mine = probs[u * 16 : u * 16 + 16]
            both = jnp.concatenate(
                [jnp.where(low_head, mine, nowhere), jnp.where(low_head, nowhere, mine)], axis=1
            )
            found = jnp.dot(both, vv[first + u].reshape(256, 128), preferred_element_type=F32)
            cf[pl.ds(first + u, 12, stride=SEQS), :] = found[0:12]

    pack(0, take_own, normed(x, scale))
    spread(0, 3)
    cross(3, 0, SLOTS)
    qf[0 : 12 * SEQS, :] = q_ref[...].astype(F32).reshape(12 * SEQS, 128)
    qf[12 * SEQS : 16 * SEQS, :] = jnp.zeros((4 * SEQS, 128), F32)
    k_copy.wait()
    v_copy.wait()
    attention(0, 4)
    weight_last = routing(route, e_last, last % SLOTS)[1]
    weight_rest = jnp.where(col // 32 == 2, 0.0, weight_own)
    rb[0, 64:96, :] = jnp.zeros((32, FEAT), BF16)
    wait(rt.at[1], rt_r)
    take_opp, weight_opp = routing(rt[1], e_col, col % SLOTS)
    attention(4, 4)
    wait(raw, raw_r)
    wait(rs.at[1], rs_r)
    pack(1, take_opp, normed(raw[...], rs[1][:, 0:1]))
    spread(0, 0)
    cross(0, 0, SLOTS)
    forward_own(3)
    attention(8, 4)
    spread(1, 3)
    spread(0, 1)
    cross(1, 0, SLOTS)
    attention(12, 4)
    forward_own(0)
    spread(1, 0)
    spread(0, 2)
    cross(2, 0, SLOTS)
    spread(1, 1)
    spread(1, 2)
    attention(16, 4)
    forward_own(1)
    forward_opp(3)
    forward_side(3)
    forward_opp(0)

    def gate_up(k, half):
        kx, cc = k // 2, k % 2
        rows = pl.ds(half * 256, 256)
        for n in range(2):
            cols = pl.ds(n * 256, 256)
            g = jnp.dot(xb[kx, cc, rows, :], wg[k, :, cols], preferred_element_type=F32)
            u = jnp.dot(xb[kx, cc, rows, :], wu[k, :, cols], preferred_element_type=F32)
            if k != 0:
                g = g + acc_g[rows, cols]
                u = u + acc_u[rows, cols]
            if k != 3:
                acc_g[rows, cols] = g
                acc_u[rows, cols] = u
            else:
                hid[rows, cols] = (g / (1.0 + jnp.exp(-g)) * u).astype(BF16)

    def weights(kind, k):
        copies[k * 3 + kind].wait()

    def down(k, half, n):
        return jnp.dot(
            hid[half * 256 : half * 256 + 256, :],
            wd[k, :, n * 512 : n * 512 + 512],
            preferred_element_type=F32,
        )

    def down_for_mate(kx, half):
        for n in range(3):
            ps[kx, half, :, n * 512 : n * 512 + 512] = down(kx * 2 + 1, half, n).astype(BF16)
        send(ps.at[kx, half], pr.at[kx, half], pr_s.at[kx, half], pr_r.at[kx, half], mate)

    def down_mine(kx, half, dst):
        wait(pr.at[kx, half], pr_r.at[kx, half])
        for n in range(3):
            cols = slice(n * 512, n * 512 + 512)
            terms = down(kx * 2, half, n) + pr[kx, half, :, cols].astype(F32)
            dst[half * 256 : half * 256 + 256, cols] = terms.astype(BF16)

    def to_sides(p):
        for h, device in ((0, near), (1, far)):
            send(
                q1.at[pl.ds(base(h, p), 64), :],
                xr.at[h, pl.ds(p * 64, 64), :],
                xq_s.at[h],
                xq_r.at[h, p],
                device,
            )

    def back_y(h, p, src, first):
        for dy in range(4):
            at = p * 64 + dy * SLOTS
            if dy == 0:
                yb[h, at : at + SLOTS, :] = src[first : first + SLOTS, :]
                continue
            send(
                src.at[pl.ds(first + dy * SLOTS, SLOTS), :],
                yb.at[h, pl.ds(at, SLOTS), :],
                r2_s.at[h],
                r2_r.at[h, p],
                plane(0, 4 - dy),
            )

    def back_z(h, p):
        wait(yb.at[h, pl.ds(p * 64 + SLOTS, 48), :], r2_r.at[h, p])
        for half in range(2):
            terms = jnp.zeros((SLOTS, FEAT), F32)
            for row in (2 * half, 2 * half + 1):
                at = p * 64 + ((row - y + 4) % 4) * SLOTS
                terms = terms + yb[h, pl.ds(pl.multiple_of(at, SLOTS), SLOTS), :].astype(F32)
            dst = rz if p != 3 else rb
            at = p * 32 + half * SLOTS
            dst[h, at : at + SLOTS, :] = terms.astype(BF16)
        if p != 3:
            rows = pl.ds(p * 32, 32)
            send(
                rz.at[h, rows, :], rb.at[h, rows, :], r3_s.at[h], r3_r.at[h], plane(4 - STEP[p], 0)
            )

    def direct(p, src, first):
        for dy in range(4):
            rows = pl.ds(dy * SLOTS, SLOTS)
            send(
                src.at[pl.ds(first + dy * SLOTS, SLOTS), :],
                rd.at[rows, :],
                rd_s,
                rd_r,
                plane(4 - STEP[p], 4 - dy),
            )

    def combine(src, weight):
        high = weight.astype(BF16)
        rest = weight - high.astype(F32)
        middle = rest.astype(BF16)
        low = (rest - middle.astype(F32)).astype(BF16)
        stacked = jnp.concatenate([high, middle, low], axis=0)
        terms = jnp.dot(stacked, src, preferred_element_type=F32)
        return terms[0:TOK] + terms[TOK : 2 * TOK] + terms[2 * TOK : 3 * TOK]

    def from_sides(p):
        rows = slice(p * 64, p * 64 + 64)
        for h in range(2):
            wait(xr.at[h, pl.ds(p * 64, 64), :], xq_r.at[h, p])
        terms = q0[base(0, p) : base(0, p) + 64, :].astype(F32)
        terms = terms + xr[0, rows, :].astype(F32) + xr[1, rows, :].astype(F32)
        own[rows, :] = terms.astype(BF16)
        if p == 2:
            direct(p, own, p * 64)
        else:
            back_y(0, p, own, p * 64)

    def from_mate(kx, half):
        wait(xb.at[kx, 1, pl.ds(half * 256, 256), :], dd_r.at[kx, half])

    for k in range(4):
        weights(0, k)
        weights(1, k)
    gate_up(0, 0)
    forward_side(0)
    from_mate(0, 0)
    gate_up(1, 0)
    forward_own(2)
    gate_up(2, 0)
    from_mate(1, 0)
    gate_up(3, 0)
    forward_opp(1)
    for k in range(4):
        weights(2, k)
    down_for_mate(1, 0)
    down_for_mate(0, 0)
    forward_opp(2)
    gate_up(0, 1)
    forward_side(1)
    down_mine(1, 0, q1)
    to_sides(0)
    to_sides(3)
    down_mine(0, 0, q0)
    back_y(1, 0, q0, base(1, 0))
    back_y(1, 3, q0, base(1, 3))
    from_mate(0, 1)
    forward_side(2)
    gate_up(1, 1)
    gate_up(2, 1)
    from_mate(1, 1)
    gate_up(3, 1)
    down_for_mate(1, 1)
    down_for_mate(0, 1)
    attention(20, 4)
    down_mine(1, 1, q1)
    to_sides(1)
    to_sides(2)
    from_sides(0)
    down_mine(0, 1, q0)
    back_y(1, 1, q0, base(1, 1))
    back_y(1, 2, q0, base(1, 2))
    back_z(1, 0)
    back_z(1, 3)
    from_sides(3)
    attention(24, 4)
    back_z(1, 1)
    back_z(0, 0)
    back_z(1, 2)
    from_sides(1)
    attention(28, 4)
    ctx_ref[...] = cf[...].reshape(12, SEQS, 128).astype(BF16)
    back_z(0, 1)
    from_sides(2)
    back_z(0, 3)
    wait(rb.at[1, pl.ds(0, 96), :], r3_r.at[1])
    fin[0] = combine(rb[1], weight_opp).astype(BF16)
    send(fin.at[0], fin.at[1], fin_s, fin_r, opp)
    wait(rb.at[0, pl.ds(0, 64), :], r3_r.at[0])
    added = combine(rb[0], weight_rest)
    wait(fin.at[1], fin_r)
    added = added + fin[1].astype(F32)
    wait(rd, rd_r)
    added = added + combine(rd[...], weight_last)
    out_ref[...] = (x_ref[...].astype(F32) + added).astype(BF16)

    wait(sq.at[pl.ds(0, 3)], sq_s)
    wait(rt.at[0], rt_s)
    wait(raw, raw_s)
    wait(rs.at[0], rs_s)
    for h in range(2):
        wait(pk.at[h, pl.ds(0, 96), :], s0_s.at[h])
        wait(xb.at[0, 0, pl.ds(0, 192), :], s1_s.at[h])
        wait(xb.at[0, 0, pl.ds(0, 256), :], xf_s.at[h])
        wait(xb.at[h, 0], dd_s.at[h])
        for half in range(2):
            wait(ps.at[h, half], pr_s.at[h, half])
        wait(xr.at[h], xq_s.at[h])
        wait(yb.at[h, pl.ds(0, 144 + 48 * h), :], r2_s.at[h])
        wait(rb.at[h, pl.ds(0, 64 + 32 * h), :], r3_s.at[h])
    wait(rd, rd_s)
    wait(fin.at[0], fin_s)


def hand_on(context_in, layer_in, context_out, layer_out):
    context_out[...] = context_in[...]
    layer_out[...] = layer_in[...]


def on_device(
    queries,
    k_cache,
    v_cache,
    lengths,
    moe_input,
    norm_gain,
    expert_ids,
    combine_weights,
    capacity,
    w_gate,
    w_up,
    w_down,
):
    vmem = pl.BlockSpec(memory_space=pltpu.VMEM)
    smem = pl.BlockSpec(memory_space=pltpu.SMEM)
    hbm = pl.BlockSpec(memory_space=pl.ANY)
    dma = pltpu.SemaphoreType.DMA
    context, layer_out = pl.pallas_call(
        kernel,
        out_shape=(
            jax.ShapeDtypeStruct((12, SEQS, 128), BF16),
            jax.ShapeDtypeStruct(moe_input.shape, BF16),
        ),
        in_specs=[smem, smem, vmem, vmem, vmem, vmem, vmem, hbm, hbm, hbm, hbm, hbm],
        out_specs=(vmem, vmem),
        scratch_shapes=[
            pltpu.VMEM((SEQS, 2, 128, 128), BF16),
            pltpu.VMEM((SEQS, 2, 128, 128), BF16),
            pltpu.VMEM((4, FEAT, HID), BF16),
            pltpu.VMEM((4, FEAT, HID), BF16),
            pltpu.VMEM((4, HID, FEAT), BF16),
            pltpu.VMEM((2, 2, ROWS, FEAT), BF16),
            pltpu.VMEM((2, 128, FEAT), BF16),
            pltpu.VMEM((2, 128, FEAT), BF16),
            pltpu.VMEM((2, 256, FEAT), BF16),
            pltpu.VMEM((2, 128, FEAT), BF16),
            pltpu.VMEM((ROWS, HID), F32),
            pltpu.VMEM((ROWS, HID), F32),
            pltpu.VMEM((ROWS, HID), BF16),
            pltpu.VMEM((2, 2, 256, FEAT), BF16),
            pltpu.VMEM((2, 2, 256, FEAT), BF16),
            pltpu.VMEM((ROWS, FEAT), BF16),
            pltpu.VMEM((ROWS, FEAT), BF16),
            pltpu.VMEM((2, 256, FEAT), BF16),
            pltpu.VMEM((256, FEAT), BF16),
            pltpu.VMEM((2, 128, FEAT), BF16),
            pltpu.VMEM((64, FEAT), BF16),
            pltpu.VMEM((4, TOK, 128), F32),
            pltpu.VMEM((2, TOK, 128), F32),
            pltpu.VMEM((TOK, FEAT), BF16),
            pltpu.VMEM((2, TOK, 128), F32),
            pltpu.VMEM((2, TOK, FEAT), BF16),
            pltpu.VMEM((16 * SEQS, 128), F32),
            pltpu.VMEM((12 * SEQS, 128), F32),
            dma((3, 4)),
            dma((2,)),
            dma,
            dma((4,)),
            dma,
            dma,
            dma,
            dma,
            dma,
            dma,
            dma((2,)),
            dma((2, 4)),
            dma((2,)),
            dma((2, 4)),
            dma((2,)),
            dma((2, 4)),
            dma((2,)),
            dma((2, 2)),
            dma((2, 2)),
            dma((2, 2)),
            dma((2,)),
            dma((2, 4)),
            dma((2,)),
            dma((2, 4)),
            dma((2,)),
            dma((2,)),
            dma,
            dma,
            dma,
            dma,
        ],
        compiler_params=pltpu.CompilerParams(
            collective_id=0, has_side_effects=True, vmem_limit_bytes=62 * 1024 * 1024
        ),
    )(
        lengths,
        capacity,
        queries.transpose(1, 0, 2),
        moe_input,
        norm_gain,
        expert_ids.T,
        combine_weights.T,
        k_cache,
        v_cache,
        w_gate,
        w_up,
        w_down,
    )
    context, layer_out = pl.pallas_call(
        hand_on,
        out_shape=(
            jax.ShapeDtypeStruct(context.shape, BF16),
            jax.ShapeDtypeStruct(layer_out.shape, BF16),
        ),
        in_specs=[vmem, vmem],
        out_specs=(vmem, vmem),
    )(context, layer_out)
    return context.transpose(1, 0, 2), layer_out


def solution(mesh):
    in_specs = (
        P("expert", "mp", None),
        P("expert", "mp", None, None),
        P("expert", "mp", None, None),
        P("expert"),
        P("expert", "mp"),
        P("mp"),
        P("expert", None),
        P("expert", None),
        P(),
        P("expert", None, "mp"),
        P("expert", None, "mp"),
        P("expert", "mp", None),
    )
    out_specs = (P("expert", "mp", None), P("expert", "mp"))
    return jax.shard_map(
        on_device, mesh=mesh, in_specs=in_specs, out_specs=out_specs, check_vma=False
    )
```
